32 devices in a mesh: row: 4 (over y, x), col: 4 (over z), fiber: 2 (over core).
Axes of the slice: x: 2, y: 2, z: 4, core: 2. Of those that a mesh axis runs over, the one named last changes fastest.
Arguments:
- user_factors: float32 [8192, 128], P(('row', 'col', 'fiber')), may hold values from -3 to 3
- item_factors: bfloat16 [16384, 128], P(('row', 'col')), may hold values from -0.119628906 to 0.119628906
- ratings: bfloat16 [4, 4, 256, 128, 128], P('row', 'col', 'fiber'), may hold values from -2 to 2, as said below
- block_user: int32 [4, 4, 256], P('row', 'col', 'fiber'), may hold values from 0 to 15, as said below
- block_item: int32 [4, 4, 256], P('row', 'col', 'fiber'), may hold values from 0 to 31, as said below
- counts: int32 [8192], P(('row', 'col', 'fiber')), may hold values from 1 to 8192, as said below
Outputs:
- factors: float32 [8192, 128], P(('row', 'col', 'fiber'))
- residual: float32 [8192, 128], P(('row', 'col', 'fiber'))
The draws below stay inside these ranges and needn't reach their ends.
Inputs may be any that keep to these rules, and one draw needn't show every extreme that they name: `block_user`: within one tile (one row index and one column index) the occupied blocks are distinct; each user block index appears in exactly 16 blocks of every tile, which fall on the two fiber halves at random. `block_item`: an item block index within the column slab. counts[u] equals the number of nonzero entries of ratings that belong to user u, over all blocks; some user has every rating of its blocks observed. Every user row of every occupied block has an observed rating; observed ratings have magnitude 0.25 or more.
All inputs are finite; a program needn't handle non-finite values.
Results may differ from the reference program's by a relative error of at most 0.012.
The reference program's roundings to bfloat16 on the way count: a program that leaves them out, or rounds other values in their place, can miss the bound.
Values may be sent and summed in bfloat16 or wider, within the bound.
A program may use at most 64 MiB of HBM per device.

```python
import jax
import jax.numpy as jnp
from jax import lax

RANK = 128
BLOCK = 128
ITERS = 2
ITEM_DEV = 1024
GRID_ROWS = 4
GRID_COLS = 4
TILE_BLOCKS = 256
USER_BLOCKS = 16
ITEM_BLOCKS = 32
BLOCKS_PER_USER = 16
USERS = 8192
ITEMS = 16384


def layout(key):
    base = jax.random.fold_in(key, 7001)
    tiles = GRID_ROWS * GRID_COLS
    perm_keys = jax.random.split(jax.random.fold_in(base, 1), tiles * USER_BLOCKS)
    perms = jax.vmap(lambda sub: jax.random.permutation(sub, ITEM_BLOCKS))(perm_keys)
    chosen = perms[:, :BLOCKS_PER_USER].reshape(tiles, TILE_BLOCKS).astype(jnp.int32)
    owners = jnp.repeat(jnp.arange(USER_BLOCKS, dtype=jnp.int32), BLOCKS_PER_USER)
    owners = jnp.broadcast_to(owners[None, :], (tiles, TILE_BLOCKS))
    order_keys = jax.random.split(jax.random.fold_in(base, 2), tiles)
    orders = jax.vmap(lambda sub: jax.random.permutation(sub, TILE_BLOCKS))(order_keys)
    users = jnp.take_along_axis(owners, orders, axis=1)
    items = jnp.take_along_axis(chosen, orders, axis=1)
    return (users.reshape(GRID_ROWS, GRID_COLS, TILE_BLOCKS), items.reshape(GRID_ROWS, GRID_COLS, TILE_BLOCKS))


def observed_entries(key):
    users, items = layout(key)
    base = jax.random.fold_in(key, 7002)
    density = jax.random.randint(jax.random.fold_in(base, 1), (USERS,), 1, 9)
    dense_user = jax.random.randint(jax.random.fold_in(base, 4), (), 0, USERS)
    density = jnp.where(jnp.arange(USERS, dtype=jnp.int32) == dense_user, 16, density)
    grid_rows = jnp.arange(GRID_ROWS, dtype=jnp.int32)[:, None, None, None]
    inside = jnp.arange(BLOCK, dtype=jnp.int32)[None, None, None, :]
    user_ids = grid_rows * (USER_BLOCKS * BLOCK) + users[..., None] * BLOCK + inside
    levels = density[user_ids]
    random_bits = jax.random.randint(jax.random.fold_in(base, 2), (GRID_ROWS, GRID_COLS, TILE_BLOCKS, BLOCK, BLOCK), 0, 16)
    forced = jax.random.randint(jax.random.fold_in(base, 3), (GRID_ROWS, GRID_COLS, TILE_BLOCKS, BLOCK), 0, BLOCK)
    column_ids = jnp.arange(BLOCK, dtype=jnp.int32)
    chosen = (random_bits < levels[..., None]) | (column_ids == forced[..., None])
    return (chosen, user_ids)


def draw_block_user(key, part):
    return layout(key)[0]


def draw_block_item(key, part):
    return layout(key)[1]


def draw_counts(key, part):
    chosen, user_ids = observed_entries(key)
    per_row = jnp.sum(chosen.astype(jnp.int32), axis=-1)
    totals = jnp.zeros((USERS,), jnp.int32)
    return totals.at[user_ids.reshape(-1)].add(per_row.reshape(-1))


def draw_ratings(key, part):
    chosen, user_ids = observed_entries(key)
    base = jax.random.fold_in(key, 7003)
    shape = (GRID_ROWS, GRID_COLS, TILE_BLOCKS, BLOCK, BLOCK)
    uniform = jax.random.uniform(jax.random.fold_in(base, 1), shape, jnp.float32)
    coins = jax.random.uniform(jax.random.fold_in(base, 2), shape, jnp.float32)
    signs = jnp.where(coins < 0.5, 1.0, -1.0)
    magnitude = 0.25 + 1.75 * uniform
    values = jnp.where(chosen, signs * magnitude, 0.0)
    return values.astype(jnp.bfloat16)


def block_scale(own_key, shape, cuts, least, top_value):
    factor_of = 1.0
    for position, shards_of in cuts:
        draws = jax.random.uniform(jax.random.fold_in(jax.random.fold_in(own_key, 6), position), (shards_of,), jnp.float32, least / len(cuts), top_value / len(cuts))
        factor_of = factor_of * jnp.repeat(jnp.exp(draws), shape[position] // shards_of).reshape((-1,) + (1,) * (len(shape) - 1 - position))
    return factor_of


def scatter_about(key, dims, spread, bound, shards=(), kind=jnp.bfloat16):
    array = spread * jax.random.normal(key, dims, jnp.float32)
    if shards:
        array = array * block_scale(key, dims, shards, -0.22, 0.18)
    return jnp.clip(array, -bound, bound).astype(kind)


def setup_inputs(seed: int = 0) -> dict:
    key_of = jax.random.split(jax.random.key(seed), 7)
    user_factors = scatter_about(key_of[0], (USERS, RANK), 0.5, 3.0, ((0, 32),), jnp.float32)
    item_factors = scatter_about(key_of[1], (ITEMS, RANK), 0.02, 0.119628906, ((0, 16),))
    ratings = draw_ratings(jax.random.fold_in(key_of[6], 71), 0)
    block_user = draw_block_user(jax.random.fold_in(key_of[6], 71), 0)
    block_item = draw_block_item(jax.random.fold_in(key_of[6], 71), 0)
    counts = draw_counts(jax.random.fold_in(key_of[6], 71), 0)
    return {"user_factors": user_factors, "item_factors": item_factors, "ratings": ratings, "block_user": block_user, "block_item": block_item, "counts": counts}


reg_weight = 4e-4
tiny = 1e-6


def block_terms(slab_values, item_slab, rating_tile, owners, columns, with_ratings):
    block_size = rating_tile.shape[1]
    factor_rank = slab_values.shape[1]
    user_count = slab_values.shape[0] // block_size
    user_rows = slab_values.reshape(user_count, block_size, factor_rank)[owners].astype(jnp.float32)
    item_rows = item_slab.reshape(item_slab.shape[0] // block_size, block_size, factor_rank)[columns].astype(jnp.float32)
    predicted = jnp.einsum("nik,njk->nij", user_rows, item_rows)
    observed = (rating_tile != 0).astype(jnp.float32)
    if with_ratings:
        weights = (rating_tile.astype(jnp.float32) - observed * predicted).astype(jnp.bfloat16)
    else:
        weights = (observed * predicted).astype(jnp.bfloat16)
    weights = lax.optimization_barrier(weights).astype(jnp.float32)
    contribution = jnp.einsum("nij,njk->nik", weights, item_rows)
    summed = jax.ops.segment_sum(contribution, owners, num_segments=user_count)
    return summed.reshape(user_count * block_size, factor_rank)


def apply_all(values, item_factors, ratings, block_user, block_item, with_ratings):
    user_grid = values.reshape(GRID_ROWS, USER_BLOCKS * BLOCK, RANK)
    item_grid = item_factors.reshape(GRID_ROWS, GRID_COLS, ITEM_DEV, RANK)
    col_index = jnp.arange(GRID_COLS, dtype=jnp.int32)

    def per_row(grid_row):
        def per_col(running, grid_col):
            item_slab = item_grid[:, grid_col].reshape(GRID_ROWS * ITEM_DEV, RANK)
            term = block_terms(user_grid[grid_row], item_slab, ratings[grid_row, grid_col], block_user[grid_row, grid_col], block_item[grid_row, grid_col], with_ratings)
            return running + term, None

        initial = jnp.zeros((USER_BLOCKS * BLOCK, RANK), jnp.float32)
        running, unused = lax.scan(per_col, initial, col_index)
        return running

    stacked = lax.map(per_row, jnp.arange(GRID_ROWS, dtype=jnp.int32))
    return stacked.reshape(USERS, RANK)


def reference(user_factors, item_factors, ratings, block_user, block_item, counts):
    damping = reg_weight * counts.astype(jnp.float32)[:, None]
    factors = user_factors
    residual = apply_all(factors.astype(jnp.bfloat16), item_factors, ratings, block_user, block_item, True) - damping * factors
    direction = residual
    squares = jnp.sum(residual * residual, axis=1, keepdims=True)
    for iteration in range(ITERS):
        image = apply_all(direction.astype(jnp.bfloat16), item_factors, ratings, block_user, block_item, False) + damping * direction
        step_size = squares / (jnp.sum(direction * image, axis=1, keepdims=True) + tiny)
        factors = factors + step_size * direction
        residual = residual - step_size * image
        if iteration + 1 < ITERS:
            renewed = jnp.sum(residual * residual, axis=1, keepdims=True)
            direction = residual + (renewed / (squares + tiny)) * direction
            squares = renewed
    return factors, residual
```

```python
import functools

import jax
import jax.numpy as jnp
from jax import lax
from jax.experimental import pallas as pl
from jax.experimental.pallas import tpu as pltpu
from jax.sharding import PartitionSpec as P

ITERS = 2
CHUNKS = 4

reg_weight = 0.0004
tiny = 1e-06

top = 32700.0
steps = 128.0
floor = 2.0**-100
pad = 16

MESH = pl.DeviceIdType.MESH


def encode(values):
    largest = jnp.maximum(jnp.max(jnp.abs(values), axis=0, keepdims=True), floor)
    level = jnp.ceil(jnp.log2(largest) * steps)
    inverse = top * jnp.exp2(level * (-1.0 / steps))
    codes = jnp.round(values * inverse).astype(jnp.int32).astype(jnp.int16)
    levels = jnp.broadcast_to(level, (pad, values.shape[1])).astype(jnp.int32).astype(jnp.int16)
    return codes, levels


def store_coded(ref, index, values):
    codes, levels = encode(values)
    size = values.shape[0]
    ref[index + (pl.ds(0, size),)] = codes
    ref[index + (pl.ds(size, pad),)] = levels


def load_coded(ref, index):
    size = ref.shape[-2] - pad
    level = ref[index + (pl.ds(size, pad),)].astype(jnp.int32).astype(jnp.float32)[:1]
    scale = jnp.exp2(level * (1.0 / steps)) * (1.0 / top)
    return ref[index + (pl.ds(0, size),)].astype(jnp.int32).astype(jnp.float32) * scale


def sweep_kernel(
    sizes, pos_ref, item_ref, uf_hbm, counts_hbm, items_hbm, ratings_hbm, x_ref, r_ref,
    vbuf, rbuf, start, pcur, part, sent, recv, tot, p_ref, res_ref, xacc, damp_ref, counts_ref,
    user_sem, count_sem, item_sem, rating_sem, v_send, v_recv, d_send, d_recv, t_send, t_recv,
    g_send, g_recv, in_send, in_recv, out_send,
):
    rows, cols, fibers = sizes
    half = cols // 2
    my_row, my_col, my_fiber = lax.axis_index("row"), lax.axis_index("col"), lax.axis_index("fiber")
    held_items = items_hbm.shape[0]
    share = held_items // fibers
    held_blocks, block = ratings_hbm.shape[0], ratings_hbm.shape[1]
    own_users = uf_hbm.shape[0] // block
    slots = cols * own_users
    per_user = pos_ref.shape[0] // slots
    chunk = held_blocks // CHUNKS

    left = 1 - lax.div(my_col, half)
    depth = left * my_col + (1 - left) * (cols - 1 - my_col)
    inner = my_col + 2 * left - 1
    outer = my_col - 2 * left + 1
    side = lax.div(depth + 1, half)

    def row_of(d):
        return lax.rem(my_row + d, rows)

    def col_of(d):
        return lax.rem(my_col + d, cols)

    def fiber_of(d):
        return lax.rem(my_fiber + d, fibers)

    item_load = pltpu.make_async_copy(items_hbm, vbuf.at[pl.ds(my_row * held_items, held_items)], item_sem)
    item_load.start()
    user_load = pltpu.make_async_copy(uf_hbm, x_ref, user_sem)
    user_load.start()
    count_load = pltpu.make_async_copy(counts_hbm, counts_ref, count_sem)
    count_load.start()

    def held_chunk(i):
        return pl.ds(my_fiber * held_blocks + i * chunk, chunk)

    rating_loads = []
    for i in range(CHUNKS):
        load = pltpu.make_async_copy(
            ratings_hbm.at[pl.ds(i * chunk, chunk)], rbuf.at[held_chunk(i)], rating_sem.at[i]
        )
        load.start()
        rating_loads.append(load)

    barrier = pltpu.get_barrier_semaphore()
    for d in range(1, rows):
        pl.semaphore_signal(barrier, inc=1, device_id={"row": row_of(d)}, device_id_type=MESH)
    for d in range(1, cols):
        pl.semaphore_signal(barrier, inc=1, device_id={"col": col_of(d)}, device_id_type=MESH)
    for d in range(1, fibers):
        pl.semaphore_signal(barrier, inc=1, device_id={"fiber": fiber_of(d)}, device_id_type=MESH)

    user_load.wait()
    for j in range(own_users):
        start[my_col * own_users + j] = x_ref[pl.ds(j * block, block), :].astype(jnp.bfloat16)
    item_load.wait()
    pl.semaphore_wait(barrier, rows + cols + fibers - 3)

    item_sends = []
    for d in range(1, rows):
        piece = pl.ds(my_row * held_items + my_fiber * share, share)
        copy = pltpu.make_async_remote_copy(
            src_ref=vbuf.at[piece],
            dst_ref=vbuf.at[piece],
            send_sem=v_send.at[d],
            recv_sem=v_recv.at[d],
            device_id={"row": row_of(d)},
            device_id_type=MESH,
        )
        copy.start()
        item_sends.append(copy)

    def start_copy(source, d, j):
        slot = source * own_users + j
        return pltpu.make_async_remote_copy(
            src_ref=start.at[slot],
            dst_ref=start.at[slot],
            send_sem=g_send.at[d, j],
            recv_sem=g_recv.at[slot],
            device_id={"col": col_of(d)},
            device_id_type=MESH,
        )

    for d in range(1, cols):
        for j in range(own_users):
            start_copy(my_col, d, j).start()
    rating_sends = []
    for i in range(CHUNKS):
        rating_loads[i].wait()
        for e in range(1, fibers):
            copy = pltpu.make_async_remote_copy(
                src_ref=rbuf.at[held_chunk(i)],
                dst_ref=rbuf.at[held_chunk(i)],
                send_sem=t_send.at[e, i],
                recv_sem=t_recv.at[e, i],
                device_id={"fiber": fiber_of(e)},
                device_id_type=MESH,
            )
            copy.start()
            rating_sends.append(copy)

    count_load.wait()
    damp_ref[...] = jnp.zeros_like(damp_ref)
    xacc[...] = jnp.zeros_like(xacc)
    for j in range(own_users):
        scaled = reg_weight * counts_ref[pl.ds(j, 1), :].astype(jnp.float32)
        across = jnp.broadcast_to(scaled, (block, block))
        own = my_col * own_users + j
        damp_ref[own] = jnp.broadcast_to(jnp.transpose(across)[:, :1], (block, damp_ref.shape[2]))
        xacc[own] = x_ref[pl.ds(j * block, block), :]

    shared = []
    for d in range(1, rows):
        item_sends[d - 1].wait_recv()
        source = lax.rem(my_row + rows - d, rows)
        piece = pl.ds(source * held_items + my_fiber * share, share)
        for e in range(1, fibers):
            copy = pltpu.make_async_remote_copy(
                src_ref=vbuf.at[piece],
                dst_ref=vbuf.at[piece],
                send_sem=d_send.at[d, e],
                recv_sem=d_recv.at[d, e],
                device_id={"fiber": fiber_of(e)},
                device_id_type=MESH,
            )
            copy.start()
            shared.append(copy)
    for copy in rating_sends + shared:
        copy.wait_recv()

    def inward(stage, u):
        return pltpu.make_async_remote_copy(
            src_ref=sent.at[stage, u],
            dst_ref=recv.at[side, stage, u],
            send_sem=in_send.at[stage, u],
            recv_sem=in_recv.at[side, stage, u],
            device_id={"col": inner},
            device_id_type=MESH,
        )

    def outward(stage, u):
        return pltpu.make_async_remote_copy(
            src_ref=tot.at[stage, u],
            dst_ref=recv.at[1, stage, u],
            send_sem=out_send.at[stage, u],
            recv_sem=in_recv.at[1, stage, u],
            device_id={"col": outer},
            device_id_type=MESH,
        )

    def arrival(which, stage, u):
        return pltpu.make_async_remote_copy(
            src_ref=sent.at[stage, u],
            dst_ref=recv.at[which, stage, u],
            send_sem=in_send.at[stage, u],
            recv_sem=in_recv.at[which, stage, u],
            device_id={"col": inner},
            device_id_type=MESH,
        )

    def terms(stage, u):
        rows_of_user = start[u] if stage == 0 else pcur[u]
        base = u * per_user
        items = jnp.concatenate([vbuf[item_ref[base + i]] for i in range(per_user)], axis=0)
        ratings = jnp.concatenate([rbuf[pos_ref[base + i]] for i in range(per_user)], axis=1)
        predicted = lax.dot_general(
            rows_of_user, items, (((1,), (1,)), ((), ())), preferred_element_type=jnp.float32
        )
        ratings = ratings.astype(jnp.float32)
        if stage == 0:
            weights = jnp.where(ratings != 0, ratings - predicted, 0.0)
        else:
            weights = jnp.where(ratings != 0, predicted, 0.0)
        total = jnp.dot(weights.astype(jnp.bfloat16), items, preferred_element_type=jnp.float32)
        if stage == 0:
            return total - damp_ref[u] * xacc[u]
        return total + damp_ref[u] * p_ref[u]

    def compute(stage, u):
        part[u] = terms(stage, u)

        @pl.when(depth == 0)
        def _():
            store_coded(sent, (stage, u), part[u])
            inward(stage, u).start()

    def pass_on(stage, u):
        @pl.when(depth > 0)
        def _():
            arrival(0, stage, u).wait_recv()
            store_coded(sent, (stage, u), part[u] + load_coded(recv, (0, stage, u)))
            inward(stage, u).start()

    def collect(stage, u):
        arrival(1, stage, u).wait_recv()

        @pl.when(depth == half - 1)
        def _():
            store_coded(tot, (stage, u), load_coded(sent, (stage, u)) + load_coded(recv, (1, stage, u)))

        @pl.when(depth < half - 1)
        def _():
            tot[stage, u] = recv[1, stage, u]

        @pl.when(depth > 0)
        def _():
            outward(stage, u).start()

    def update(stage, u):
        image = load_coded(tot, (stage, u))
        if stage == 0:
            res_ref[u] = image
            p_ref[u] = image
            pcur[u] = image.astype(jnp.bfloat16)
            return
        direction = p_ref[u]
        residual = res_ref[u]
        square = jnp.sum(residual * residual, axis=1, keepdims=True)
        step_size = square / (jnp.sum(direction * image, axis=1, keepdims=True) + tiny)
        residual = residual - step_size * image
        res_ref[u] = residual
        xacc[u] = xacc[u] + step_size * direction
        if stage < ITERS:
            renewed = jnp.sum(residual * residual, axis=1, keepdims=True)
            direction = residual + renewed / (square + tiny) * direction
            p_ref[u] = direction
            pcur[u] = direction.astype(jnp.bfloat16)

    order = sorted(range(cols), key=lambda c: (abs(2 * c - cols + 1), c))
    order = [c * own_users + j for c in order for j in range(own_users)]
    for u in order:
        @pl.when(my_col != u // own_users)
        def _():
            start_copy(u // own_users, 1, u % own_users).wait_recv()

        compute(0, u)
    for u in order:
        pass_on(0, u)
    for stage in range(ITERS):
        for u in order:
            collect(stage, u)
            update(stage, u)
            compute(stage + 1, u)
        for u in order:
            pass_on(stage + 1, u)
    for u in order:
        collect(ITERS, u)
    for j in range(own_users):
        own = my_col * own_users + j
        update(ITERS, own)
        users = pl.ds(j * block, block)
        x_ref[users, :] = xacc[own]
        r_ref[users, :] = res_ref[own]

    for copy in item_sends + rating_sends + shared:
        copy.wait_send()
    for d in range(1, cols):
        for j in range(own_users):
            start_copy(my_col, d, j).wait_send()
    for stage in range(ITERS + 1):
        for u in order:
            inward(stage, u).wait_send()

    @pl.when(depth > 0)
    def _():
        for stage in range(ITERS + 1):
            for u in order:
                outward(stage, u).wait_send()


def per_device(sizes, slab_users, user_factors, item_factors, ratings, block_user, block_item, counts):
    rows, cols, fibers = sizes
    held_blocks, block = ratings.shape[2], ratings.shape[3]
    rank = user_factors.shape[1]
    users = user_factors.shape[0]
    own_users = users // block
    item_blocks = item_factors.shape[0] // block
    per_user = fibers * held_blocks // (slab_users // block)

    both = lax.all_gather(jnp.stack([block_user[0, 0], block_item[0, 0]]), "fiber", axis=0)
    owners = both[:, 0].reshape(-1)
    columns = both[:, 1].reshape(-1)
    here = jnp.arange(owners.shape[0], dtype=jnp.int32)
    keys = owners * owners.shape[0] + here
    ranks = jnp.sum((keys[None, :] < keys[:, None]).astype(jnp.int32), axis=1)
    groups = jnp.arange(cols, dtype=jnp.int32)[:, None] * fibers + lax.axis_index("fiber")
    wanted = (
        groups[:, :, None] * (own_users * per_user)
        + jnp.arange(own_users * per_user, dtype=jnp.int32)[None, None, :]
    ).reshape(-1)
    match = wanted[:, None] == ranks[None, :]
    positions = jnp.sum(jnp.where(match, here[None, :], 0), axis=1)
    items = jnp.sum(jnp.where(match, columns[None, :], 0), axis=1)

    stages = ITERS + 1
    slots = cols * own_users
    dma = pltpu.SemaphoreType.DMA
    vmem = pl.BlockSpec(memory_space=pltpu.VMEM)
    smem = pl.BlockSpec(memory_space=pltpu.SMEM)
    hbm = pl.BlockSpec(memory_space=pl.ANY)
    return pl.pallas_call(
        functools.partial(sweep_kernel, sizes),
        out_shape=(
            jax.ShapeDtypeStruct((users, rank), jnp.float32),
            jax.ShapeDtypeStruct((users, rank), jnp.float32),
        ),
        in_specs=[smem, smem, hbm, hbm, hbm, hbm],
        out_specs=(vmem, vmem),
        scratch_shapes=[
            pltpu.VMEM((rows * item_blocks, block, rank), jnp.bfloat16),
            pltpu.VMEM((fibers * held_blocks, block, block), jnp.bfloat16),
            pltpu.VMEM((slots, block, rank), jnp.bfloat16),
            pltpu.VMEM((slots, block, rank), jnp.bfloat16),
            pltpu.VMEM((slots, block, rank), jnp.float32),
            pltpu.VMEM((stages, slots, block + pad, rank), jnp.int16),
            pltpu.VMEM((2, stages, slots, block + pad, rank), jnp.int16),
            pltpu.VMEM((stages, slots, block + pad, rank), jnp.int16),
            pltpu.VMEM((slots, block, rank), jnp.float32),
            pltpu.VMEM((slots, block, rank), jnp.float32),
            pltpu.VMEM((slots, block, rank), jnp.float32),
            pltpu.VMEM((slots, block, rank), jnp.float32),
            pltpu.VMEM((own_users, block), jnp.int32),
            dma,
            dma,
            dma,
            dma((CHUNKS,)),
            dma((rows,)),
            dma((rows,)),
            dma((rows, fibers)),
            dma((rows, fibers)),
            dma((fibers, CHUNKS)),
            dma((fibers, CHUNKS)),
            dma((cols, own_users)),
            dma((slots,)),
            dma((stages, slots)),
            dma((2, stages, slots)),
            dma((stages, slots)),
        ],
        compiler_params=pltpu.CompilerParams(
            collective_id=0, has_side_effects=True, vmem_limit_bytes=67043328
        ),
    )(
        positions,
        items,
        user_factors,
        counts.reshape(own_users, block),
        item_factors.reshape(item_blocks, block, rank),
        ratings[0, 0],
    )


def solution(mesh):
    sizes = (mesh.shape["row"], mesh.shape["col"], mesh.shape["fiber"])

    def whole(user_factors, item_factors, ratings, block_user, block_item, counts):
        slab_users = user_factors.shape[0] // sizes[0]
        return jax.shard_map(
            functools.partial(per_device, sizes, slab_users),
            mesh=mesh,
            in_specs=(
                P(("row", "col", "fiber"), None),
                P(("row", "col"), None),
                P("row", "col", "fiber", None, None),
                P("row", "col", "fiber"),
                P("row", "col", "fiber"),
                P(("row", "col", "fiber")),
            ),
            out_specs=(P(("row", "col", "fiber"), None), P(("row", "col", "fiber"), None)),
            check_vma=False,
        )(user_factors, item_factors, ratings, block_user, block_item, counts)

    return whole
```

```python
import functools

import jax
import jax.numpy as jnp
from jax import lax
from jax.experimental import pallas as pl
from jax.experimental.pallas import tpu as pltpu
from jax.sharding import PartitionSpec as P

ITERS = 2
CHUNKS = 4
LAG = 3

reg_weight = 0.0004
tiny = 1e-06

top = 32700.0
steps = 128.0
floor = 2.0**-100
pad = 16

MESH = pl.DeviceIdType.MESH


def encode(values):
    largest = jnp.maximum(jnp.max(jnp.abs(values), axis=0, keepdims=True), floor)
    level = jnp.ceil(jnp.log2(largest) * steps)
    inverse = top * jnp.exp2(level * (-1.0 / steps))
    codes = jnp.round(values * inverse).astype(jnp.int32).astype(jnp.int16)
    levels = jnp.broadcast_to(level, (pad, values.shape[1])).astype(jnp.int32).astype(jnp.int16)
    return codes, levels


def store_coded(ref, index, values):
    codes, levels = encode(values)
    size = values.shape[0]
    ref[index + (pl.ds(0, size),)] = codes
    ref[index + (pl.ds(size, pad),)] = levels


def load_coded(ref, index):
    size = ref.shape[-2] - pad
    level = ref[index + (pl.ds(size, pad),)].astype(jnp.int32).astype(jnp.float32)[:1]
    scale = jnp.exp2(level * (1.0 / steps)) * (1.0 / top)
    return ref[index + (pl.ds(0, size),)].astype(jnp.int32).astype(jnp.float32) * scale


def sweep_kernel(
    sizes, owner_hbm, column_hbm, uf_hbm, counts_hbm, items_hbm, ratings_hbm, x_ref, r_ref,
    vbuf, rbuf, start, pcur, part, sent, recv, tot, last, p_ref, res_ref, xacc, damp_ref, counts_ref,
    ids, places, pos_ref, user_sem, count_sem, id_sem, place_sem, item_sem, rating_sem, i_send, i_recv,
    v_send, v_recv, d_send, d_recv, t_send, t_recv,
    g_send, g_recv, in_send, in_recv, out_send, f_send, f_recv,
):
    rows, cols, fibers = sizes
    half = cols // 2
    my_row, my_col, my_fiber = lax.axis_index("row"), lax.axis_index("col"), lax.axis_index("fiber")
    held_items = items_hbm.shape[0]
    share = held_items // fibers
    parts = 2 if rows == 4 and share % 2 == 0 else 1
    piece = share // parts
    held_blocks, block = ratings_hbm.shape[0], ratings_hbm.shape[1]
    own_users = uf_hbm.shape[0] // block
    slots = cols * own_users
    per_user = pos_ref.shape[1] // slots
    chunk = held_blocks // CHUNKS

    left = 1 - lax.div(my_col, half)
    depth = left * my_col + (1 - left) * (cols - 1 - my_col)
    inner = my_col + 2 * left - 1
    outer = my_col - 2 * left + 1
    side = lax.div(depth + 1, half)

    def row_of(d):
        return lax.rem(my_row + d, rows)

    def col_of(d):
        return lax.rem(my_col + d, cols)

    def fiber_of(d):
        return lax.rem(my_fiber + d, fibers)

    id_loads = [
        pltpu.make_async_copy(source, ids.at[my_fiber, i], id_sem.at[i])
        for i, source in enumerate((owner_hbm, column_hbm))
    ]
    for load in id_loads:
        load.start()
    item_load = pltpu.make_async_copy(items_hbm, vbuf.at[pl.ds(my_row * held_items, held_items)], item_sem)
    item_load.start()
    user_load = pltpu.make_async_copy(uf_hbm, x_ref, user_sem)
    user_load.start()
    count_load = pltpu.make_async_copy(counts_hbm, counts_ref, count_sem)
    count_load.start()

    def held_chunk(i):
        return pl.ds(my_fiber * held_blocks + i * chunk, chunk)

    rating_loads = []
    for i in range(CHUNKS):
        load = pltpu.make_async_copy(
            ratings_hbm.at[pl.ds(i * chunk, chunk)], rbuf.at[held_chunk(i)], rating_sem.at[i]
        )
        load.start()
        rating_loads.append(load)

    barrier = pltpu.get_barrier_semaphore()
    for d in range(1, rows):
        pl.semaphore_signal(barrier, inc=1, device_id={"row": row_of(d)}, device_id_type=MESH)
    for d in range(1, cols):
        pl.semaphore_signal(barrier, inc=1, device_id={"col": col_of(d)}, device_id_type=MESH)
    for d in range(1, fibers):
        pl.semaphore_signal(barrier, inc=1, device_id={"fiber": fiber_of(d)}, device_id_type=MESH)

    user_load.wait()
    for j in range(own_users):
        start[my_col * own_users + j] = x_ref[pl.ds(j * block, block), :].astype(jnp.bfloat16)
    for load in id_loads:
        load.wait()
    item_load.wait()
    pl.semaphore_wait(barrier, rows + cols + fibers - 3)

    id_sends = []
    for e in range(1, fibers):
        copy = pltpu.make_async_remote_copy(
            src_ref=ids.at[my_fiber],
            dst_ref=ids.at[my_fiber],
            send_sem=i_send.at[e],
            recv_sem=i_recv.at[e],
            device_id={"fiber": fiber_of(e)},
            device_id_type=MESH,
        )
        copy.start()
        id_sends.append(copy)

    def item_piece(row, i):
        return pl.ds(row * held_items + my_fiber * share + i * piece, piece)

    def item_copy(source, d, i, target):
        return pltpu.make_async_remote_copy(
            src_ref=vbuf.at[item_piece(source, i)],
            dst_ref=vbuf.at[item_piece(source, i)],
            send_sem=v_send.at[d, i],
            recv_sem=v_recv.at[d, i],
            device_id={"row": target},
            device_id_type=MESH,
        )

    if parts == 2:
        across = my_row + 1 - 2 * lax.rem(my_row, 2)
        along = my_row + 2 - 4 * lax.div(my_row, 2)
        corner = 3 - my_row
        peers = [my_row, across, along, corner]
        first = [item_copy(my_row, 1, 0, across), item_copy(my_row, 2, 1, along)]
        first += [item_copy(my_row, 1, 1, across), item_copy(my_row, 2, 0, along)]
        relays = [
            (item_copy(across, 1, 0, across), item_copy(across, 3, 0, along)),
            (item_copy(along, 2, 1, along), item_copy(along, 3, 1, across)),
        ]
        landed = [(1, 1), (2, 0), (3, 0), (3, 1)]
    else:
        peers = [lax.rem(my_row + rows - d, rows) for d in range(rows)]
        first = [item_copy(my_row, d, 0, row_of(d)) for d in range(1, rows)]
        relays = []
        landed = [(d, 0) for d in range(1, rows)]
    for copy in first:
        copy.start()
    item_sends = first + [onward for _, onward in relays]

    def start_copy(source, d, j):
        slot = source * own_users + j
        return pltpu.make_async_remote_copy(
            src_ref=start.at[slot],
            dst_ref=start.at[slot],
            send_sem=g_send.at[d, j],
            recv_sem=g_recv.at[slot],
            device_id={"col": col_of(d)},
            device_id_type=MESH,
        )

    for d in range(1, cols):
        for j in range(own_users):
            start_copy(my_col, d, j).start()
    rating_sends = []
    for i in range(CHUNKS):
        rating_loads[i].wait()
        for e in range(1, fibers):
            copy = pltpu.make_async_remote_copy(
                src_ref=rbuf.at[held_chunk(i)],
                dst_ref=rbuf.at[held_chunk(i)],
                send_sem=t_send.at[e, i],
                recv_sem=t_recv.at[e, i],
                device_id={"fiber": fiber_of(e)},
                device_id_type=MESH,
            )
            copy.start()
            rating_sends.append(copy)

    count_load.wait()
    damp_ref[...] = jnp.zeros_like(damp_ref)
    xacc[...] = jnp.zeros_like(xacc)
    for j in range(own_users):
        scaled = reg_weight * counts_ref[pl.ds(j, 1), :].astype(jnp.float32)
        across = jnp.broadcast_to(scaled, (block, block))
        own = my_col * own_users + j
        damp_ref[own] = jnp.broadcast_to(jnp.transpose(across)[:, :1], (block, damp_ref.shape[2]))
        xacc[own] = x_ref[pl.ds(j * block, block), :]

    for copy in id_sends:
        copy.wait_recv()
    total_blocks = fibers * held_blocks
    lanes = (held_blocks, held_blocks)
    here = lax.broadcasted_iota(jnp.int32, lanes, 0)
    lane = lax.broadcasted_iota(jnp.int32, lanes, 1)
    group = own_users * per_user
    ahead = sum(jnp.where(lane >= c * group, 1, 0) for c in range(1, cols))
    wanted = lane + (ahead * (fibers - 1) + my_fiber) * group
    keys = [jnp.broadcast_to(ids[e, 0], lanes) * total_blocks + lane + e * held_blocks for e in range(fibers)]
    standing = [jnp.transpose(key) for key in keys]
    found_place = jnp.zeros((1, held_blocks), jnp.int32)
    found_item = jnp.zeros((1, held_blocks), jnp.int32)
    for e in range(fibers):
        before = sum(jnp.where(other < keys[e], 1, 0) for other in standing)
        rank = jnp.sum(before, axis=0, keepdims=True)
        match = jnp.transpose(jnp.broadcast_to(rank, lanes)) == wanted
        column = jnp.transpose(jnp.broadcast_to(ids[e, 1], lanes))
        found_place += jnp.sum(jnp.where(match, here + e * held_blocks, 0), axis=0, keepdims=True)
        found_item += jnp.sum(jnp.where(match, column, 0), axis=0, keepdims=True)
    places[0:1, :] = found_place
    places[1:2, :] = found_item
    place_copy = pltpu.make_async_copy(places, pos_ref, place_sem)
    place_copy.start()

    shared = []

    def share_piece(d, i):
        for e in range(1, fibers):
            copy = pltpu.make_async_remote_copy(
                src_ref=vbuf.at[item_piece(peers[d], i)],
                dst_ref=vbuf.at[item_piece(peers[d], i)],
                send_sem=d_send.at[d, i, e],
                recv_sem=d_recv.at[d, i, e],
                device_id={"fiber": fiber_of(e)},
                device_id_type=MESH,
            )
            copy.start()
            shared.append(copy)

    for arrived, onward in relays:
        arrived.wait_recv()
        onward.start()
    if parts == 2:
        share_piece(1, 0)
        share_piece(2, 1)
    for d, i in landed:
        item_copy(peers[d], d, i, my_row).wait_recv()
        share_piece(d, i)
    place_copy.wait()
    for copy in rating_sends + shared:
        copy.wait_recv()

    def inward(stage, u):
        return pltpu.make_async_remote_copy(
            src_ref=sent.at[stage, u],
            dst_ref=recv.at[side, stage, u],
            send_sem=in_send.at[stage, u],
            recv_sem=in_recv.at[side, stage, u],
            device_id={"col": inner},
            device_id_type=MESH,
        )

    def outward(stage, u):
        return pltpu.make_async_remote_copy(
            src_ref=tot.at[stage, u],
            dst_ref=recv.at[1, stage, u],
            send_sem=out_send.at[stage, u],
            recv_sem=in_recv.at[1, stage, u],
            device_id={"col": outer},
            device_id_type=MESH,
        )

    def arrival(which, stage, u):
        return pltpu.make_async_remote_copy(
            src_ref=sent.at[stage, u],
            dst_ref=recv.at[which, stage, u],
            send_sem=in_send.at[stage, u],
            recv_sem=in_recv.at[which, stage, u],
            device_id={"col": inner},
            device_id_type=MESH,
        )

    def terms(stage, u):
        rows_of_user = start[u] if stage == 0 else pcur[u]
        base = u * per_user
        items = jnp.concatenate([vbuf[pos_ref[1, base + i]] for i in range(per_user)], axis=0)
        ratings = jnp.concatenate([rbuf[pos_ref[0, base + i]] for i in range(per_user)], axis=1)
        predicted = lax.dot_general(
            rows_of_user, items, (((1,), (1,)), ((), ())), preferred_element_type=jnp.float32
        )
        ratings = ratings.astype(jnp.float32)
        if stage == 0:
            weights = jnp.where(ratings != 0, ratings - predicted, 0.0)
        else:
            weights = jnp.where(ratings != 0, predicted, 0.0)
        total = jnp.dot(weights.astype(jnp.bfloat16), items, preferred_element_type=jnp.float32)
        if stage == 0:
            return total - damp_ref[u] * xacc[u]
        return total + damp_ref[u] * p_ref[u]

    def deliver(d, j, target, source):
        return pltpu.make_async_remote_copy(
            src_ref=sent.at[ITERS, target * own_users + j],
            dst_ref=last.at[source, j],
            send_sem=f_send.at[d, j],
            recv_sem=f_recv.at[source, j],
            device_id={"col": target},
            device_id_type=MESH,
        )

    def compute(stage, u):
        part[u] = terms(stage, u)
        if stage == ITERS:
            @pl.when(my_col != u // own_users)
            def _():
                store_coded(sent, (stage, u), part[u])
                deliver(u // own_users, u % own_users, u // own_users, my_col).start()

            return

        @pl.when(depth == 0)
        def _():
            store_coded(sent, (stage, u), part[u])
            inward(stage, u).start()

    def pass_on(stage, u):
        @pl.when(depth > 0)
        def _():
            arrival(0, stage, u).wait_recv()
            store_coded(sent, (stage, u), part[u] + load_coded(recv, (0, stage, u)))
            inward(stage, u).start()

    def collect(stage, u):
        arrival(1, stage, u).wait_recv()

        @pl.when(depth == half - 1)
        def _():
            store_coded(tot, (stage, u), load_coded(sent, (stage, u)) + load_coded(recv, (1, stage, u)))

        @pl.when(depth < half - 1)
        def _():
            tot[stage, u] = recv[1, stage, u]

        @pl.when(depth > 0)
        def _():
            outward(stage, u).start()

    def update(stage, u, image=None):
        if stage < ITERS:
            image = load_coded(tot, (stage, u))
        if stage == 0:
            res_ref[u] = image
            p_ref[u] = image
            pcur[u] = image.astype(jnp.bfloat16)
            return
        direction = p_ref[u]
        residual = res_ref[u]
        square = jnp.sum(residual * residual, axis=1, keepdims=True)
        step_size = square / (jnp.sum(direction * image, axis=1, keepdims=True) + tiny)
        residual = residual - step_size * image
        res_ref[u] = residual
        xacc[u] = xacc[u] + step_size * direction
        if stage < ITERS:
            renewed = jnp.sum(residual * residual, axis=1, keepdims=True)
            direction = residual + renewed / (square + tiny) * direction
            p_ref[u] = direction
            pcur[u] = direction.astype(jnp.bfloat16)

    order = sorted(range(cols), key=lambda c: (abs(2 * c - cols + 1), c))
    order = [c * own_users + j for c in order for j in range(own_users)]
    for u in order:
        @pl.when(my_col != u // own_users)
        def _():
            start_copy(u // own_users, 1, u % own_users).wait_recv()

        compute(0, u)
    for stage in range(ITERS):
        for step in range(slots + LAG):
            if step < slots:
                pass_on(stage, order[step])
            if step >= LAG:
                u = order[step - LAG]
                collect(stage, u)
                update(stage, u)
                compute(stage + 1, u)
    for j in range(own_users):
        own = my_col * own_users + j
        image = part[own]
        for d in range(1, cols):
            source = col_of(d)
            deliver(d, j, my_col, source).wait_recv()
            image = image + load_coded(last, (source, j))
        update(ITERS, own, image)
        users = pl.ds(j * block, block)
        x_ref[users, :] = xacc[own]
        r_ref[users, :] = res_ref[own]

    for copy in item_sends + rating_sends + shared + id_sends:
        copy.wait_send()
    for d in range(1, cols):
        for j in range(own_users):
            start_copy(my_col, d, j).wait_send()
            deliver(col_of(d), j, col_of(d), my_col).wait_send()
    for stage in range(ITERS):
        for u in order:
            inward(stage, u).wait_send()

    @pl.when(depth > 0)
    def _():
        for stage in range(ITERS):
            for u in order:
                outward(stage, u).wait_send()


def per_device(sizes, user_factors, item_factors, ratings, block_user, block_item, counts):
    rows, cols, fibers = sizes
    held_blocks, block = ratings.shape[2], ratings.shape[3]
    rank = user_factors.shape[1]
    users = user_factors.shape[0]
    own_users = users // block
    item_blocks = item_factors.shape[0] // block

    stages = ITERS + 1
    slots = cols * own_users
    dma = pltpu.SemaphoreType.DMA
    vmem = pl.BlockSpec(memory_space=pltpu.VMEM)
    hbm = pl.BlockSpec(memory_space=pl.ANY)
    return hand_out(*pl.pallas_call(
        functools.partial(sweep_kernel, sizes),
        out_shape=(
            jax.ShapeDtypeStruct((users, rank), jnp.float32),
            jax.ShapeDtypeStruct((users, rank), jnp.float32),
        ),
        in_specs=[hbm] * 6,
        out_specs=(vmem, vmem),
        scratch_shapes=[
            pltpu.VMEM((rows * item_blocks, block, rank), jnp.bfloat16),
            pltpu.VMEM((fibers * held_blocks, block, block), jnp.bfloat16),
            pltpu.VMEM((slots, block, rank), jnp.bfloat16),
            pltpu.VMEM((slots, block, rank), jnp.bfloat16),
            pltpu.VMEM((slots, block, rank), jnp.float32),
            pltpu.VMEM((stages, slots, block + pad, rank), jnp.int16),
            pltpu.VMEM((2, ITERS, slots, block + pad, rank), jnp.int16),
            pltpu.VMEM((ITERS, slots, block + pad, rank), jnp.int16),
            pltpu.VMEM((cols, own_users, block + pad, rank), jnp.int16),
            pltpu.VMEM((slots, block, rank), jnp.float32),
            pltpu.VMEM((slots, block, rank), jnp.float32),
            pltpu.VMEM((slots, block, rank), jnp.float32),
            pltpu.VMEM((slots, block, rank), jnp.float32),
            pltpu.VMEM((own_users, block), jnp.int32),
            pltpu.VMEM((fibers, 2, 1, held_blocks), jnp.int32),
            pltpu.VMEM((2, held_blocks), jnp.int32),
            pltpu.SMEM((2, held_blocks), jnp.int32),
            dma,
            dma,
            dma((2,)),
            dma,
            dma,
            dma((CHUNKS,)),
            dma((fibers,)),
            dma((fibers,)),
            dma((rows, 2)),
            dma((rows, 2)),
            dma((rows, 2, fibers)),
            dma((rows, 2, fibers)),
            dma((fibers, CHUNKS)),
            dma((fibers, CHUNKS)),
            dma((cols, own_users)),
            dma((slots,)),
            dma((ITERS, slots)),
            dma((2, ITERS, slots)),
            dma((ITERS, slots)),
            dma((cols, own_users)),
            dma((cols, own_users)),
        ],
        compiler_params=pltpu.CompilerParams(
            collective_id=0, has_side_effects=True, vmem_limit_bytes=67043328
        ),
    )(
        block_user[0],
        block_item[0],
        user_factors,
        counts.reshape(own_users, block),
        item_factors.reshape(item_blocks, block, rank),
        ratings[0, 0],
    ))


def tail_kernel(x_ref, r_ref, xo_ref, ro_ref, sems):
    a = pltpu.make_async_copy(x_ref, xo_ref, sems.at[0])
    b = pltpu.make_async_copy(r_ref, ro_ref, sems.at[1])
    a.start()
    b.start()
    a.wait()
    b.wait()


def hand_out(x, r):
    vmem = pl.BlockSpec(memory_space=pltpu.VMEM)
    hbm = pl.BlockSpec(memory_space=pl.ANY)
    return pl.pallas_call(
        tail_kernel,
        out_shape=(jax.ShapeDtypeStruct(x.shape, x.dtype), jax.ShapeDtypeStruct(r.shape, r.dtype)),
        in_specs=[vmem, vmem],
        out_specs=(hbm, hbm),
        scratch_shapes=[pltpu.SemaphoreType.DMA((2,))],
    )(x, r)


def solution(mesh):
    sizes = (mesh.shape["row"], mesh.shape["col"], mesh.shape["fiber"])

    def whole(user_factors, item_factors, ratings, block_user, block_item, counts):
        return jax.shard_map(
            functools.partial(per_device, sizes),
            mesh=mesh,
            in_specs=(
                P(("row", "col", "fiber"), None),
                P(("row", "col"), None),
                P("row", "col", "fiber", None, None),
                P("row", "col", "fiber"),
                P("row", "col", "fiber"),
                P(("row", "col", "fiber")),
            ),
            out_specs=(P(("row", "col", "fiber"), None), P(("row", "col", "fiber"), None)),
            check_vma=False,
        )(user_factors, item_factors, ratings, block_user, block_item, counts)

    return whole
```

```python
import functools

import jax
import jax.numpy as jnp
from jax import lax
from jax.experimental import pallas as pl
from jax.experimental.pallas import tpu as pltpu
from jax.sharding import PartitionSpec as P

ITERS = 2
CHUNKS = 4
LAG = 3

reg_weight = 0.0004
tiny = 1e-06

top = 32700.0
steps = 128.0
floor = 2.0**-100
pad = 8

MESH = pl.DeviceIdType.MESH


def encode(values):
    largest = jnp.maximum(jnp.max(jnp.abs(values), axis=0, keepdims=True), floor)
    level = jnp.ceil(jnp.log2(largest) * steps)
    inverse = top * jnp.exp2(level * (-1.0 / steps))
    codes = jnp.round(values * inverse).astype(jnp.int32).astype(jnp.int16)
    levels = jnp.broadcast_to(level, (pad, values.shape[1])).astype(jnp.int32).astype(jnp.int16)
    return codes, levels


def store_coded(ref, index, values):
    codes, levels = encode(values)
    size = values.shape[0]
    ref[index + (pl.ds(0, size),)] = codes
    ref[index + (pl.ds(size, pad),)] = levels


def load_coded(ref, index):
    size = ref.shape[-2] - pad
    level = ref[index + (pl.ds(size, pad),)].astype(jnp.int32).astype(jnp.float32)[:1]
    scale = jnp.exp2(level * (1.0 / steps)) * (1.0 / top)
    return ref[index + (pl.ds(0, size),)].astype(jnp.int32).astype(jnp.float32) * scale


def sweep_kernel(
    sizes, owner_hbm, column_hbm, uf_hbm, counts_hbm, items_hbm, ratings_hbm, x_ref, r_ref,
    vbuf, rbuf, start, pcur, part, sent, recv, tot, last, p_ref, res_ref, xacc, damp_ref, counts_ref,
    ids, places, pos_ref, user_sem, count_sem, id_sem, place_sem, item_sem, rating_sem, i_send, i_recv,
    v_send, v_recv, d_send, d_recv, t_send, t_recv,
    g_send, g_recv, in_send, in_recv, out_send, f_send, f_recv,
):
    rows, cols, fibers = sizes
    half = cols // 2
    my_row, my_col, my_fiber = lax.axis_index("row"), lax.axis_index("col"), lax.axis_index("fiber")
    held_items = items_hbm.shape[0]
    share = held_items // fibers
    parts = 2 if rows == 4 and share % 2 == 0 else 1
    piece = share // parts
    held_blocks, block = ratings_hbm.shape[0], ratings_hbm.shape[1]
    own_users = uf_hbm.shape[0] // block
    slots = cols * own_users
    per_user = pos_ref.shape[1] // slots
    chunk = held_blocks // CHUNKS

    left = 1 - lax.div(my_col, half)
    depth = left * my_col + (1 - left) * (cols - 1 - my_col)
    inner = my_col + 2 * left - 1
    outer = my_col - 2 * left + 1
    side = lax.div(depth + 1, half)

    def row_of(d):
        return lax.rem(my_row + d, rows)

    def col_of(d):
        return lax.rem(my_col + d, cols)

    def fiber_of(d):
        return lax.rem(my_fiber + d, fibers)

    id_loads = [
        pltpu.make_async_copy(source, ids.at[my_fiber, i], id_sem.at[i])
        for i, source in enumerate((owner_hbm, column_hbm))
    ]
    for load in id_loads:
        load.start()
    item_load = pltpu.make_async_copy(items_hbm, vbuf.at[pl.ds(my_row * held_items, held_items)], item_sem)
    item_load.start()
    user_load = pltpu.make_async_copy(uf_hbm, x_ref, user_sem)
    user_load.start()
    count_load = pltpu.make_async_copy(counts_hbm, counts_ref, count_sem)
    count_load.start()

    def held_chunk(i):
        return pl.ds(my_fiber * held_blocks + i * chunk, chunk)

    rating_loads = []
    for i in range(CHUNKS):
        load = pltpu.make_async_copy(
            ratings_hbm.at[pl.ds(i * chunk, chunk)], rbuf.at[held_chunk(i)], rating_sem.at[i]
        )
        load.start()
        rating_loads.append(load)

    barrier = pltpu.get_barrier_semaphore()
    for d in range(1, rows):
        pl.semaphore_signal(barrier, inc=1, device_id={"row": row_of(d)}, device_id_type=MESH)
    for d in range(1, cols):
        pl.semaphore_signal(barrier, inc=1, device_id={"col": col_of(d)}, device_id_type=MESH)
    for d in range(1, fibers):
        pl.semaphore_signal(barrier, inc=1, device_id={"fiber": fiber_of(d)}, device_id_type=MESH)

    user_load.wait()
    for j in range(own_users):
        start[my_col * own_users + j] = x_ref[pl.ds(j * block, block), :].astype(jnp.bfloat16)
    for load in id_loads:
        load.wait()
    item_load.wait()
    pl.semaphore_wait(barrier, rows + cols + fibers - 3)

    id_sends = []
    for e in range(1, fibers):
        copy = pltpu.make_async_remote_copy(
            src_ref=ids.at[my_fiber],
            dst_ref=ids.at[my_fiber],
            send_sem=i_send.at[e],
            recv_sem=i_recv.at[e],
            device_id={"fiber": fiber_of(e)},
            device_id_type=MESH,
        )
        copy.start()
        id_sends.append(copy)

    def item_piece(row, i):
        return pl.ds(row * held_items + my_fiber * share + i * piece, piece)

    def item_copy(source, d, i, target):
        return pltpu.make_async_remote_copy(
            src_ref=vbuf.at[item_piece(source, i)],
            dst_ref=vbuf.at[item_piece(source, i)],
            send_sem=v_send.at[d, i],
            recv_sem=v_recv.at[d, i],
            device_id={"row": target},
            device_id_type=MESH,
        )

    if parts == 2:
        across = my_row + 1 - 2 * lax.rem(my_row, 2)
        along = my_row + 2 - 4 * lax.div(my_row, 2)
        corner = 3 - my_row
        peers = [my_row, across, along, corner]
        first = [item_copy(my_row, 1, 0, across), item_copy(my_row, 2, 1, along)]
        first += [item_copy(my_row, 1, 1, across), item_copy(my_row, 2, 0, along)]
        relays = [
            (item_copy(across, 1, 0, across), item_copy(across, 3, 0, along)),
            (item_copy(along, 2, 1, along), item_copy(along, 3, 1, across)),
        ]
        landed = [(1, 1), (2, 0), (3, 0), (3, 1)]
    else:
        peers = [lax.rem(my_row + rows - d, rows) for d in range(rows)]
        first = [item_copy(my_row, d, 0, row_of(d)) for d in range(1, rows)]
        relays = []
        landed = [(d, 0) for d in range(1, rows)]
    for copy in first:
        copy.start()
    item_sends = first + [onward for _, onward in relays]

    def start_copy(source, d, j):
        slot = source * own_users + j
        return pltpu.make_async_remote_copy(
            src_ref=start.at[slot],
            dst_ref=start.at[slot],
            send_sem=g_send.at[d, j],
            recv_sem=g_recv.at[slot],
            device_id={"col": col_of(d)},
            device_id_type=MESH,
        )

    for d in range(1, cols):
        for j in range(own_users):
            start_copy(my_col, d, j).start()
    rating_sends = []
    for i in range(CHUNKS):
        rating_loads[i].wait()
        for e in range(1, fibers):
            copy = pltpu.make_async_remote_copy(
                src_ref=rbuf.at[held_chunk(i)],
                dst_ref=rbuf.at[held_chunk(i)],
                send_sem=t_send.at[e, i],
                recv_sem=t_recv.at[e, i],
                device_id={"fiber": fiber_of(e)},
                device_id_type=MESH,
            )
            copy.start()
            rating_sends.append(copy)

    count_load.wait()
    damp_ref[...] = jnp.zeros_like(damp_ref)
    xacc[...] = jnp.zeros_like(xacc)
    for j in range(own_users):
        scaled = reg_weight * counts_ref[pl.ds(j, 1), :].astype(jnp.float32)
        across = jnp.broadcast_to(scaled, (block, block))
        own = my_col * own_users + j
        damp_ref[own] = jnp.broadcast_to(jnp.transpose(across)[:, :1], (block, damp_ref.shape[2]))
        xacc[own] = x_ref[pl.ds(j * block, block), :]

    for copy in id_sends:
        copy.wait_recv()
    total_blocks = fibers * held_blocks
    lanes = (held_blocks, held_blocks)
    here = lax.broadcasted_iota(jnp.int32, lanes, 0)
    lane = lax.broadcasted_iota(jnp.int32, lanes, 1)
    group = own_users * per_user
    ahead = sum(jnp.where(lane >= c * group, 1, 0) for c in range(1, cols))
    wanted = lane + (ahead * (fibers - 1) + my_fiber) * group
    keys = [jnp.broadcast_to(ids[e, 0], lanes) * total_blocks + lane + e * held_blocks for e in range(fibers)]
    standing = [jnp.transpose(key) for key in keys]
    found_place = jnp.zeros((1, held_blocks), jnp.int32)
    found_item = jnp.zeros((1, held_blocks), jnp.int32)
    for e in range(fibers):
        before = sum(jnp.where(other < keys[e], 1, 0) for other in standing)
        rank = jnp.sum(before, axis=0, keepdims=True)
        match = jnp.transpose(jnp.broadcast_to(rank, lanes)) == wanted
        column = jnp.transpose(jnp.broadcast_to(ids[e, 1], lanes))
        found_place += jnp.sum(jnp.where(match, here + e * held_blocks, 0), axis=0, keepdims=True)
        found_item += jnp.sum(jnp.where(match, column, 0), axis=0, keepdims=True)
    places[0:1, :] = found_place
    places[1:2, :] = found_item
    place_copy = pltpu.make_async_copy(places, pos_ref, place_sem)
    place_copy.start()

    shared = []

    def share_piece(d, i):
        for e in range(1, fibers):
            copy = pltpu.make_async_remote_copy(
                src_ref=vbuf.at[item_piece(peers[d], i)],
                dst_ref=vbuf.at[item_piece(peers[d], i)],
                send_sem=d_send.at[d, i, e],
                recv_sem=d_recv.at[d, i, e],
                device_id={"fiber": fiber_of(e)},
                device_id_type=MESH,
            )
            copy.start()
            shared.append(copy)

    for arrived, onward in relays:
        arrived.wait_recv()
        onward.start()
    if parts == 2:
        share_piece(1, 0)
        share_piece(2, 1)
    for d, i in landed:
        item_copy(peers[d], d, i, my_row).wait_recv()
        share_piece(d, i)
    place_copy.wait()
    for copy in rating_sends + shared:
        copy.wait_recv()

    def inward(stage, u):
        return pltpu.make_async_remote_copy(
            src_ref=sent.at[stage, u],
            dst_ref=recv.at[side, stage, u],
            send_sem=in_send.at[stage, u],
            recv_sem=in_recv.at[side, stage, u],
            device_id={"col": inner},
            device_id_type=MESH,
        )

    def outward(stage, u):
        return pltpu.make_async_remote_copy(
            src_ref=tot.at[stage, u],
            dst_ref=recv.at[1, stage, u],
            send_sem=out_send.at[stage, u],
            recv_sem=in_recv.at[1, stage, u],
            device_id={"col": outer},
            device_id_type=MESH,
        )

    def arrival(which, stage, u):
        return pltpu.make_async_remote_copy(
            src_ref=sent.at[stage, u],
            dst_ref=recv.at[which, stage, u],
            send_sem=in_send.at[stage, u],
            recv_sem=in_recv.at[which, stage, u],
            device_id={"col": inner},
            device_id_type=MESH,
        )

    def terms(stage, u):
        rows_of_user = start[u] if stage == 0 else pcur[u]
        base = u * per_user
        items = jnp.concatenate([vbuf[pos_ref[1, base + i]] for i in range(per_user)], axis=0)
        ratings = jnp.concatenate([rbuf[pos_ref[0, base + i]] for i in range(per_user)], axis=1)
        predicted = lax.dot_general(
            rows_of_user, items, (((1,), (1,)), ((), ())), preferred_element_type=jnp.float32
        )
        ratings = ratings.astype(jnp.float32)
        if stage == 0:
            weights = jnp.where(ratings != 0, ratings - predicted, 0.0)
        else:
            weights = jnp.where(ratings != 0, predicted, 0.0)
        total = jnp.dot(weights.astype(jnp.bfloat16), items, preferred_element_type=jnp.float32)
        if stage == 0:
            return total - damp_ref[u] * xacc[u]
        return total + damp_ref[u] * p_ref[u]

    def deliver(d, j, target, source):
        return pltpu.make_async_remote_copy(
            src_ref=sent.at[ITERS, target * own_users + j],
            dst_ref=last.at[source, j],
            send_sem=f_send.at[d, j],
            recv_sem=f_recv.at[source, j],
            device_id={"col": target},
            device_id_type=MESH,
        )

    def compute(stage, u):
        part[u] = terms(stage, u)
        if stage == ITERS:
            @pl.when(my_col != u // own_users)
            def _():
                store_coded(sent, (stage, u), part[u])
                deliver(u // own_users, u % own_users, u // own_users, my_col).start()

            return

        @pl.when(depth == 0)
        def _():
            store_coded(sent, (stage, u), part[u])
            inward(stage, u).start()

    def pass_on(stage, u):
        @pl.when(depth > 0)
        def _():
            arrival(0, stage, u).wait_recv()
            store_coded(sent, (stage, u), part[u] + load_coded(recv, (0, stage, u)))
            inward(stage, u).start()

    def collect(stage, u):
        arrival(1, stage, u).wait_recv()

        @pl.when(depth == half - 1)
        def _():
            store_coded(tot, (stage, u), load_coded(sent, (stage, u)) + load_coded(recv, (1, stage, u)))

        @pl.when(depth < half - 1)
        def _():
            tot[stage, u] = recv[1, stage, u]

        @pl.when(depth > 0)
        def _():
            outward(stage, u).start()

    def update(stage, u, image=None):
        if stage < ITERS:
            image = load_coded(tot, (stage, u))
        if stage == 0:
            res_ref[u] = image
            p_ref[u] = image
            pcur[u] = image.astype(jnp.bfloat16)
            return
        direction = p_ref[u]
        residual = res_ref[u]
        square = jnp.sum(residual * residual, axis=1, keepdims=True)
        step_size = square / (jnp.sum(direction * image, axis=1, keepdims=True) + tiny)
        residual = residual - step_size * image
        res_ref[u] = residual
        xacc[u] = xacc[u] + step_size * direction
        if stage < ITERS:
            renewed = jnp.sum(residual * residual, axis=1, keepdims=True)
            direction = residual + renewed / (square + tiny) * direction
            p_ref[u] = direction
            pcur[u] = direction.astype(jnp.bfloat16)

    order = sorted(range(cols), key=lambda c: (-abs(2 * c - cols + 1), c))
    order = [c * own_users + j for c in order for j in range(own_users)]
    for u in order:
        @pl.when(my_col != u // own_users)
        def _():
            start_copy(u // own_users, 1, u % own_users).wait_recv()

        compute(0, u)
    for stage in range(ITERS):
        for step in range(slots + LAG):
            if step < slots:
                pass_on(stage, order[step])
            if step >= LAG:
                u = order[step - LAG]
                collect(stage, u)
                update(stage, u)
                compute(stage + 1, u)
    for j in range(own_users):
        own = my_col * own_users + j
        image = part[own]
        for d in range(1, cols):
            source = col_of(d)
            deliver(d, j, my_col, source).wait_recv()
            image = image + load_coded(last, (source, j))
        update(ITERS, own, image)
        users = pl.ds(j * block, block)
        x_ref[users, :] = xacc[own]
        r_ref[users, :] = res_ref[own]

    for copy in item_sends + rating_sends + shared + id_sends:
        copy.wait_send()
    for d in range(1, cols):
        for j in range(own_users):
            start_copy(my_col, d, j).wait_send()
            deliver(col_of(d), j, col_of(d), my_col).wait_send()
    for stage in range(ITERS):
        for u in order:
            inward(stage, u).wait_send()

    @pl.when(depth > 0)
    def _():
        for stage in range(ITERS):
            for u in order:
                outward(stage, u).wait_send()


def per_device(sizes, user_factors, item_factors, ratings, block_user, block_item, counts):
    rows, cols, fibers = sizes
    held_blocks, block = ratings.shape[2], ratings.shape[3]
    rank = user_factors.shape[1]
    users = user_factors.shape[0]
    own_users = users // block
    item_blocks = item_factors.shape[0] // block

    stages = ITERS + 1
    slots = cols * own_users
    dma = pltpu.SemaphoreType.DMA
    vmem = pl.BlockSpec(memory_space=pltpu.VMEM)
    hbm = pl.BlockSpec(memory_space=pl.ANY)
    return hand_out(*pl.pallas_call(
        functools.partial(sweep_kernel, sizes),
        out_shape=(
            jax.ShapeDtypeStruct((users, rank), jnp.float32),
            jax.ShapeDtypeStruct((users, rank), jnp.float32),
        ),
        in_specs=[hbm] * 6,
        out_specs=(vmem, vmem),
        scratch_shapes=[
            pltpu.VMEM((rows * item_blocks, block, rank), jnp.bfloat16),
            pltpu.VMEM((fibers * held_blocks, block, block), jnp.bfloat16),
            pltpu.VMEM((slots, block, rank), jnp.bfloat16),
            pltpu.VMEM((slots, block, rank), jnp.bfloat16),
            pltpu.VMEM((slots, block, rank), jnp.float32),
            pltpu.VMEM((stages, slots, block + pad, rank), jnp.int16),
            pltpu.VMEM((2, ITERS, slots, block + pad, rank), jnp.int16),
            pltpu.VMEM((ITERS, slots, block + pad, rank), jnp.int16),
            pltpu.VMEM((cols, own_users, block + pad, rank), jnp.int16),
            pltpu.VMEM((slots, block, rank), jnp.float32),
            pltpu.VMEM((slots, block, rank), jnp.float32),
            pltpu.VMEM((slots, block, rank), jnp.float32),
            pltpu.VMEM((slots, block, rank), jnp.float32),
            pltpu.VMEM((own_users, block), jnp.int32),
            pltpu.VMEM((fibers, 2, 1, held_blocks), jnp.int32),
            pltpu.VMEM((2, held_blocks), jnp.int32),
            pltpu.SMEM((2, held_blocks), jnp.int32),
            dma,
            dma,
            dma((2,)),
            dma,
            dma,
            dma((CHUNKS,)),
            dma((fibers,)),
            dma((fibers,)),
            dma((rows, 2)),
            dma((rows, 2)),
            dma((rows, 2, fibers)),
            dma((rows, 2, fibers)),
            dma((fibers, CHUNKS)),
            dma((fibers, CHUNKS)),
            dma((cols, own_users)),
            dma((slots,)),
            dma((ITERS, slots)),
            dma((2, ITERS, slots)),
            dma((ITERS, slots)),
            dma((cols, own_users)),
            dma((cols, own_users)),
        ],
        compiler_params=pltpu.CompilerParams(
            collective_id=0, has_side_effects=True, vmem_limit_bytes=67043328
        ),
    )(
        block_user[0],
        block_item[0],
        user_factors,
        counts.reshape(own_users, block),
        item_factors.reshape(item_blocks, block, rank),
        ratings[0, 0],
    ))


def tail_kernel(x_ref, r_ref, xo_ref, ro_ref, sems):
    a = pltpu.make_async_copy(x_ref, xo_ref, sems.at[0])
    b = pltpu.make_async_copy(r_ref, ro_ref, sems.at[1])
    a.start()
    b.start()
    a.wait()
    b.wait()


def hand_out(x, r):
    vmem = pl.BlockSpec(memory_space=pltpu.VMEM)
    hbm = pl.BlockSpec(memory_space=pl.ANY)
    return pl.pallas_call(
        tail_kernel,
        out_shape=(jax.ShapeDtypeStruct(x.shape, x.dtype), jax.ShapeDtypeStruct(r.shape, r.dtype)),
        in_specs=[vmem, vmem],
        out_specs=(hbm, hbm),
        scratch_shapes=[pltpu.SemaphoreType.DMA((2,))],
    )(x, r)


def solution(mesh):
    sizes = (mesh.shape["row"], mesh.shape["col"], mesh.shape["fiber"])

    def whole(user_factors, item_factors, ratings, block_user, block_item, counts):
        return jax.shard_map(
            functools.partial(per_device, sizes),
            mesh=mesh,
            in_specs=(
                P(("row", "col", "fiber"), None),
                P(("row", "col"), None),
                P("row", "col", "fiber", None, None),
                P("row", "col", "fiber"),
                P("row", "col", "fiber"),
                P(("row", "col", "fiber")),
            ),
            out_specs=(P(("row", "col", "fiber"), None), P(("row", "col", "fiber"), None)),
            check_vma=False,
        )(user_factors, item_factors, ratings, block_user, block_item, counts)

    return whole
```

```python
import functools

import jax
import jax.numpy as jnp
from jax import lax
from jax.experimental import pallas as pl
from jax.experimental.pallas import tpu as pltpu
from jax.sharding import PartitionSpec as P

ITERS = 2
CHUNKS = 2
LAG = 3

reg_weight = 0.0004
tiny = 1e-06

top = 32700.0
steps = 128.0
floor = 2.0**-100
pad = 8

MESH = pl.DeviceIdType.MESH


def encode(values):
    largest = jnp.maximum(jnp.max(jnp.abs(values), axis=0, keepdims=True), floor)
    level = jnp.ceil(jnp.log2(largest) * steps)
    inverse = top * jnp.exp2(level * (-1.0 / steps))
    codes = jnp.round(values * inverse).astype(jnp.int32).astype(jnp.int16)
    levels = jnp.broadcast_to(level, (pad, values.shape[1])).astype(jnp.int32).astype(jnp.int16)
    return codes, levels


def store_coded(ref, index, values):
    codes, levels = encode(values)
    size = values.shape[0]
    ref[index + (pl.ds(0, size),)] = codes
    ref[index + (pl.ds(size, pad),)] = levels


def load_coded(ref, index):
    size = ref.shape[-2] - pad
    level = ref[index + (pl.ds(size, pad),)].astype(jnp.int32).astype(jnp.float32)[:1]
    scale = jnp.exp2(level * (1.0 / steps)) * (1.0 / top)
    return ref[index + (pl.ds(0, size),)].astype(jnp.int32).astype(jnp.float32) * scale


def sweep_kernel(
    sizes, owner_hbm, column_hbm, uf_hbm, counts_hbm, items_hbm, ratings_hbm, x_ref, r_ref,
    vbuf, rbuf, start, pcur, part, sent, recv, tot, last, p_ref, res_ref, xacc, damp_ref, counts_ref,
    ids, places, pos_ref, user_sem, count_sem, id_sem, place_sem, item_sem, rating_sem, i_send, i_recv,
    v_send, v_recv, d_send, d_recv, t_send, t_recv,
    g_send, g_recv, in_send, in_recv, out_send, f_send, f_recv,
):
    rows, cols, fibers = sizes
    half = cols // 2
    my_row, my_col, my_fiber = lax.axis_index("row"), lax.axis_index("col"), lax.axis_index("fiber")
    held_items = items_hbm.shape[0]
    share = held_items // fibers
    parts = 2 if rows == 4 and share % 2 == 0 else 1
    piece = share // parts
    held_blocks, block = ratings_hbm.shape[0], ratings_hbm.shape[1]
    own_users = uf_hbm.shape[0] // block
    slots = cols * own_users
    per_user = pos_ref.shape[1] // slots
    chunk = held_blocks // CHUNKS

    left = 1 - lax.div(my_col, half)
    depth = left * my_col + (1 - left) * (cols - 1 - my_col)
    inner = my_col + 2 * left - 1
    outer = my_col - 2 * left + 1
    side = lax.div(depth + 1, half)

    def row_of(d):
        return lax.rem(my_row + d, rows)

    def col_of(d):
        return lax.rem(my_col + d, cols)

    def fiber_of(d):
        return lax.rem(my_fiber + d, fibers)

    id_loads = [
        pltpu.make_async_copy(source, ids.at[my_fiber, i], id_sem.at[i])
        for i, source in enumerate((owner_hbm, column_hbm))
    ]
    for load in id_loads:
        load.start()
    item_load = pltpu.make_async_copy(items_hbm, vbuf.at[pl.ds(my_row * held_items, held_items)], item_sem)
    item_load.start()
    user_load = pltpu.make_async_copy(uf_hbm, x_ref, user_sem)
    user_load.start()
    count_load = pltpu.make_async_copy(counts_hbm, counts_ref, count_sem)
    count_load.start()

    def held_chunk(i):
        return pl.ds(my_fiber * held_blocks + i * chunk, chunk)

    rating_loads = []
    for i in range(CHUNKS):
        load = pltpu.make_async_copy(
            ratings_hbm.at[pl.ds(i * chunk, chunk)], rbuf.at[held_chunk(i)], rating_sem.at[i]
        )
        load.start()
        rating_loads.append(load)

    barrier = pltpu.get_barrier_semaphore()
    for d in range(1, rows):
        pl.semaphore_signal(barrier, inc=1, device_id={"row": row_of(d)}, device_id_type=MESH)
    for d in range(1, cols):
        pl.semaphore_signal(barrier, inc=1, device_id={"col": col_of(d)}, device_id_type=MESH)
    for d in range(1, fibers):
        pl.semaphore_signal(barrier, inc=1, device_id={"fiber": fiber_of(d)}, device_id_type=MESH)

    user_load.wait()
    for j in range(own_users):
        start[my_col * own_users + j] = x_ref[pl.ds(j * block, block), :].astype(jnp.bfloat16)
    for load in id_loads:
        load.wait()
    item_load.wait()
    pl.semaphore_wait(barrier, rows + cols + fibers - 3)

    id_sends = []
    for e in range(1, fibers):
        copy = pltpu.make_async_remote_copy(
            src_ref=ids.at[my_fiber],
            dst_ref=ids.at[my_fiber],
            send_sem=i_send.at[e],
            recv_sem=i_recv.at[e],
            device_id={"fiber": fiber_of(e)},
            device_id_type=MESH,
        )
        copy.start()
        id_sends.append(copy)

    def item_piece(row, i):
        return pl.ds(row * held_items + my_fiber * share + i * piece, piece)

    def item_copy(source, d, i, target):
        return pltpu.make_async_remote_copy(
            src_ref=vbuf.at[item_piece(source, i)],
            dst_ref=vbuf.at[item_piece(source, i)],
            send_sem=v_send.at[d, i],
            recv_sem=v_recv.at[d, i],
            device_id={"row": target},
            device_id_type=MESH,
        )

    if parts == 2:
        across = my_row + 1 - 2 * lax.rem(my_row, 2)
        along = my_row + 2 - 4 * lax.div(my_row, 2)
        corner = 3 - my_row
        peers = [my_row, across, along, corner]
        first = [item_copy(my_row, 1, 0, across), item_copy(my_row, 2, 1, along)]
        first += [item_copy(my_row, 1, 1, across), item_copy(my_row, 2, 0, along)]
        relays = [
            (item_copy(across, 1, 0, across), item_copy(across, 3, 0, along)),
            (item_copy(along, 2, 1, along), item_copy(along, 3, 1, across)),
        ]
        landed = [(1, 1), (2, 0), (3, 0), (3, 1)]
    else:
        peers = [lax.rem(my_row + rows - d, rows) for d in range(rows)]
        first = [item_copy(my_row, d, 0, row_of(d)) for d in range(1, rows)]
        relays = []
        landed = [(d, 0) for d in range(1, rows)]
    for copy in first:
        copy.start()
    item_sends = first + [onward for _, onward in relays]

    def start_copy(source, d, j):
        slot = source * own_users + j
        return pltpu.make_async_remote_copy(
            src_ref=start.at[slot],
            dst_ref=start.at[slot],
            send_sem=g_send.at[d, j],
            recv_sem=g_recv.at[slot],
            device_id={"col": col_of(d)},
            device_id_type=MESH,
        )

    for d in range(1, cols):
        for j in range(own_users):
            start_copy(my_col, d, j).start()
    rating_sends = []
    for i in range(CHUNKS):
        rating_loads[i].wait()
        for e in range(1, fibers):
            copy = pltpu.make_async_remote_copy(
                src_ref=rbuf.at[held_chunk(i)],
                dst_ref=rbuf.at[held_chunk(i)],
                send_sem=t_send.at[e, i],
                recv_sem=t_recv.at[e, i],
                device_id={"fiber": fiber_of(e)},
                device_id_type=MESH,
            )
            copy.start()
            rating_sends.append(copy)

    count_load.wait()
    damp_ref[...] = jnp.zeros_like(damp_ref)
    xacc[...] = jnp.zeros_like(xacc)
    for j in range(own_users):
        scaled = reg_weight * counts_ref[pl.ds(j, 1), :].astype(jnp.float32)
        across = jnp.broadcast_to(scaled, (block, block))
        own = my_col * own_users + j
        damp_ref[own] = jnp.broadcast_to(jnp.transpose(across)[:, :1], (block, damp_ref.shape[2]))
        xacc[own] = x_ref[pl.ds(j * block, block), :]

    for copy in id_sends:
        copy.wait_recv()
    total_blocks = fibers * held_blocks
    lanes = (held_blocks, held_blocks)
    here = lax.broadcasted_iota(jnp.int32, lanes, 0)
    lane = lax.broadcasted_iota(jnp.int32, lanes, 1)
    group = own_users * per_user
    ahead = sum(jnp.where(lane >= c * group, 1, 0) for c in range(1, cols))
    wanted = lane + (ahead * (fibers - 1) + my_fiber) * group
    keys = [jnp.broadcast_to(ids[e, 0], lanes) * total_blocks + lane + e * held_blocks for e in range(fibers)]
    standing = [jnp.transpose(key) for key in keys]
    found_place = jnp.zeros((1, held_blocks), jnp.int32)
    found_item = jnp.zeros((1, held_blocks), jnp.int32)
    for e in range(fibers):
        before = sum(jnp.where(other < keys[e], 1, 0) for other in standing)
        rank = jnp.sum(before, axis=0, keepdims=True)
        match = jnp.transpose(jnp.broadcast_to(rank, lanes)) == wanted
        column = jnp.transpose(jnp.broadcast_to(ids[e, 1], lanes))
        found_place += jnp.sum(jnp.where(match, here + e * held_blocks, 0), axis=0, keepdims=True)
        found_item += jnp.sum(jnp.where(match, column, 0), axis=0, keepdims=True)
    places[0:1, :] = found_place
    places[1:2, :] = found_item
    place_copy = pltpu.make_async_copy(places, pos_ref, place_sem)
    place_copy.start()

    shared = []

    def share_piece(d, i):
        for e in range(1, fibers):
            copy = pltpu.make_async_remote_copy(
                src_ref=vbuf.at[item_piece(peers[d], i)],
                dst_ref=vbuf.at[item_piece(peers[d], i)],
                send_sem=d_send.at[d, i, e],
                recv_sem=d_recv.at[d, i, e],
                device_id={"fiber": fiber_of(e)},
                device_id_type=MESH,
            )
            copy.start()
            shared.append(copy)

    for arrived, onward in relays:
        arrived.wait_recv()
        onward.start()
    if parts == 2:
        share_piece(1, 0)
        share_piece(2, 1)
    for d, i in landed:
        item_copy(peers[d], d, i, my_row).wait_recv()
        share_piece(d, i)
    place_copy.wait()
    for copy in rating_sends + shared:
        copy.wait_recv()

    def inward(stage, u):
        return pltpu.make_async_remote_copy(
            src_ref=sent.at[stage, u],
            dst_ref=recv.at[side, stage, u],
            send_sem=in_send.at[stage, u],
            recv_sem=in_recv.at[side, stage, u],
            device_id={"col": inner},
            device_id_type=MESH,
        )

    def outward(stage, u):
        return pltpu.make_async_remote_copy(
            src_ref=tot.at[stage, u],
            dst_ref=recv.at[1, stage, u],
            send_sem=out_send.at[stage, u],
            recv_sem=in_recv.at[1, stage, u],
            device_id={"col": outer},
            device_id_type=MESH,
        )

    def arrival(which, stage, u):
        return pltpu.make_async_remote_copy(
            src_ref=sent.at[stage, u],
            dst_ref=recv.at[which, stage, u],
            send_sem=in_send.at[stage, u],
            recv_sem=in_recv.at[which, stage, u],
            device_id={"col": inner},
            device_id_type=MESH,
        )

    def terms(stage, u):
        rows_of_user = start[u] if stage == 0 else pcur[u]
        base = u * per_user
        items = jnp.concatenate([vbuf[pos_ref[1, base + i]] for i in range(per_user)], axis=0)
        ratings = jnp.concatenate([rbuf[pos_ref[0, base + i]] for i in range(per_user)], axis=1)
        predicted = lax.dot_general(
            rows_of_user, items, (((1,), (1,)), ((), ())), preferred_element_type=jnp.float32
        )
        ratings = ratings.astype(jnp.float32)
        if stage == 0:
            weights = jnp.where(ratings != 0, ratings - predicted, 0.0)
        else:
            weights = jnp.where(ratings != 0, predicted, 0.0)
        total = jnp.dot(weights.astype(jnp.bfloat16), items, preferred_element_type=jnp.float32)
        if stage == 0:
            return total - damp_ref[u] * xacc[u]
        return total + damp_ref[u] * p_ref[u]

    def deliver(d, j, target, source):
        return pltpu.make_async_remote_copy(
            src_ref=sent.at[ITERS, target * own_users + j],
            dst_ref=last.at[source, j],
            send_sem=f_send.at[d, j],
            recv_sem=f_recv.at[source, j],
            device_id={"col": target},
            device_id_type=MESH,
        )

    def compute(stage, u):
        part[u] = terms(stage, u)
        if stage == ITERS:
            @pl.when(my_col != u // own_users)
            def _():
                store_coded(sent, (stage, u), part[u])
                deliver(u // own_users, u % own_users, u // own_users, my_col).start()

            return

        @pl.when(depth == 0)
        def _():
            store_coded(sent, (stage, u), part[u])
            inward(stage, u).start()

    def pass_on(stage, u):
        @pl.when(depth > 0)
        def _():
            arrival(0, stage, u).wait_recv()
            store_coded(sent, (stage, u), part[u] + load_coded(recv, (0, stage, u)))
            inward(stage, u).start()

    def collect(stage, u):
        arrival(1, stage, u).wait_recv()

        @pl.when(depth == half - 1)
        def _():
            store_coded(tot, (stage, u), load_coded(sent, (stage, u)) + load_coded(recv, (1, stage, u)))

        @pl.when(depth < half - 1)
        def _():
            tot[stage, u] = recv[1, stage, u]

        @pl.when(depth > 0)
        def _():
            outward(stage, u).start()

    def update(stage, u, image=None):
        if stage < ITERS:
            image = load_coded(tot, (stage, u))
        if stage == 0:
            res_ref[u] = image
            p_ref[u] = image
            pcur[u] = image.astype(jnp.bfloat16)
            return
        direction = p_ref[u]
        residual = res_ref[u]
        square = jnp.sum(residual * residual, axis=1, keepdims=True)
        step_size = square / (jnp.sum(direction * image, axis=1, keepdims=True) + tiny)
        residual = residual - step_size * image
        res_ref[u] = residual
        xacc[u] = xacc[u] + step_size * direction
        if stage < ITERS:
            renewed = jnp.sum(residual * residual, axis=1, keepdims=True)
            direction = residual + renewed / (square + tiny) * direction
            p_ref[u] = direction
            pcur[u] = direction.astype(jnp.bfloat16)

    order = sorted(range(cols), key=lambda c: (-abs(2 * c - cols + 1), c))
    order = [c * own_users + j for j in range(own_users) for c in order]
    for u in order:
        @pl.when(my_col != u // own_users)
        def _():
            start_copy(u // own_users, 1, u % own_users).wait_recv()

        compute(0, u)
    for stage in range(ITERS):
        for step in range(slots + LAG):
            if step < slots:
                pass_on(stage, order[step])
            if step >= LAG:
                u = order[step - LAG]
                collect(stage, u)
                update(stage, u)
                compute(stage + 1, u)
    for j in range(own_users):
        own = my_col * own_users + j
        image = part[own]
        for d in range(1, cols):
            source = col_of(d)
            deliver(d, j, my_col, source).wait_recv()
            image = image + load_coded(last, (source, j))
        update(ITERS, own, image)
        users = pl.ds(j * block, block)
        x_ref[users, :] = xacc[own]
        r_ref[users, :] = res_ref[own]

    for copy in item_sends + rating_sends + shared + id_sends:
        copy.wait_send()
    for d in range(1, cols):
        for j in range(own_users):
            start_copy(my_col, d, j).wait_send()
            deliver(col_of(d), j, col_of(d), my_col).wait_send()
    for stage in range(ITERS):
        for u in order:
            inward(stage, u).wait_send()

    @pl.when(depth > 0)
    def _():
        for stage in range(ITERS):
            for u in order:
                outward(stage, u).wait_send()


def per_device(sizes, user_factors, item_factors, ratings, block_user, block_item, counts):
    rows, cols, fibers = sizes
    held_blocks, block = ratings.shape[2], ratings.shape[3]
    rank = user_factors.shape[1]
    users = user_factors.shape[0]
    own_users = users // block
    item_blocks = item_factors.shape[0] // block

    stages = ITERS + 1
    slots = cols * own_users
    dma = pltpu.SemaphoreType.DMA
    vmem = pl.BlockSpec(memory_space=pltpu.VMEM)
    hbm = pl.BlockSpec(memory_space=pl.ANY)
    return hand_out(*pl.pallas_call(
        functools.partial(sweep_kernel, sizes),
        out_shape=(
            jax.ShapeDtypeStruct((users, rank), jnp.float32),
            jax.ShapeDtypeStruct((users, rank), jnp.float32),
        ),
        in_specs=[hbm] * 6,
        out_specs=(vmem, vmem),
        scratch_shapes=[
            pltpu.VMEM((rows * item_blocks, block, rank), jnp.bfloat16),
            pltpu.VMEM((fibers * held_blocks, block, block), jnp.bfloat16),
            pltpu.VMEM((slots, block, rank), jnp.bfloat16),
            pltpu.VMEM((slots, block, rank), jnp.bfloat16),
            pltpu.VMEM((slots, block, rank), jnp.float32),
            pltpu.VMEM((stages, slots, block + pad, rank), jnp.int16),
            pltpu.VMEM((2, ITERS, slots, block + pad, rank), jnp.int16),
            pltpu.VMEM((ITERS, slots, block + pad, rank), jnp.int16),
            pltpu.VMEM((cols, own_users, block + pad, rank), jnp.int16),
            pltpu.VMEM((slots, block, rank), jnp.float32),
            pltpu.VMEM((slots, block, rank), jnp.float32),
            pltpu.VMEM((slots, block, rank), jnp.float32),
            pltpu.VMEM((slots, block, rank), jnp.float32),
            pltpu.VMEM((own_users, block), jnp.int32),
            pltpu.VMEM((fibers, 2, 1, held_blocks), jnp.int32),
            pltpu.VMEM((2, held_blocks), jnp.int32),
            pltpu.SMEM((2, held_blocks), jnp.int32),
            dma,
            dma,
            dma((2,)),
            dma,
            dma,
            dma((CHUNKS,)),
            dma((fibers,)),
            dma((fibers,)),
            dma((rows, 2)),
            dma((rows, 2)),
            dma((rows, 2, fibers)),
            dma((rows, 2, fibers)),
            dma((fibers, CHUNKS)),
            dma((fibers, CHUNKS)),
            dma((cols, own_users)),
            dma((slots,)),
            dma((ITERS, slots)),
            dma((2, ITERS, slots)),
            dma((ITERS, slots)),
            dma((cols, own_users)),
            dma((cols, own_users)),
        ],
        compiler_params=pltpu.CompilerParams(
            collective_id=0, has_side_effects=True, vmem_limit_bytes=67043328
        ),
    )(
        block_user[0],
        block_item[0],
        user_factors,
        counts.reshape(own_users, block),
        item_factors.reshape(item_blocks, block, rank),
        ratings[0, 0],
    ))


def tail_kernel(x_ref, r_ref, xo_ref, ro_ref, sems):
    a = pltpu.make_async_copy(x_ref, xo_ref, sems.at[0])
    b = pltpu.make_async_copy(r_ref, ro_ref, sems.at[1])
    a.start()
    b.start()
    a.wait()
    b.wait()


def hand_out(x, r):
    vmem = pl.BlockSpec(memory_space=pltpu.VMEM)
    hbm = pl.BlockSpec(memory_space=pl.ANY)
    return pl.pallas_call(
        tail_kernel,
        out_shape=(jax.ShapeDtypeStruct(x.shape, x.dtype), jax.ShapeDtypeStruct(r.shape, r.dtype)),
        in_specs=[vmem, vmem],
        out_specs=(hbm, hbm),
        scratch_shapes=[pltpu.SemaphoreType.DMA((2,))],
    )(x, r)


def solution(mesh):
    sizes = (mesh.shape["row"], mesh.shape["col"], mesh.shape["fiber"])

    def whole(user_factors, item_factors, ratings, block_user, block_item, counts):
        return jax.shard_map(
            functools.partial(per_device, sizes),
            mesh=mesh,
            in_specs=(
                P(("row", "col", "fiber"), None),
                P(("row", "col"), None),
                P("row", "col", "fiber", None, None),
                P("row", "col", "fiber"),
                P("row", "col", "fiber"),
                P(("row", "col", "fiber")),
            ),
            out_specs=(P(("row", "col", "fiber"), None), P(("row", "col", "fiber"), None)),
            check_vma=False,
        )(user_factors, item_factors, ratings, block_user, block_item, counts)

    return whole
```

```python
import functools

import jax
import jax.numpy as jnp
from jax import lax
from jax.experimental import pallas as pl
from jax.experimental.pallas import tpu as pltpu
from jax.sharding import PartitionSpec as P

ITERS = 2
CHUNKS = 2
LAG = 3
CUTS = 1

reg_weight = 0.0004
tiny = 1e-06

top = 32700.0
steps = 128.0
floor = 2.0**-100
pad = 8

MESH = pl.DeviceIdType.MESH


def encode(values):
    largest = jnp.maximum(jnp.max(jnp.abs(values), axis=0, keepdims=True), floor)
    level = jnp.ceil(jnp.log2(largest) * steps)
    inverse = top * jnp.exp2(level * (-1.0 / steps))
    codes = jnp.round(values * inverse).astype(jnp.int32).astype(jnp.int16)
    levels = jnp.broadcast_to(level, (pad, values.shape[1])).astype(jnp.int32).astype(jnp.int16)
    return codes, levels


def store_coded(ref, index, values):
    codes, levels = encode(values)
    size = values.shape[0]
    ref[index + (pl.ds(0, size),)] = codes
    ref[index + (pl.ds(size, pad),)] = levels


def load_coded(ref, index):
    size = ref.shape[-2] - pad
    level = ref[index + (pl.ds(size, pad),)].astype(jnp.int32).astype(jnp.float32)[:1]
    scale = jnp.exp2(level * (1.0 / steps)) * (1.0 / top)
    return ref[index + (pl.ds(0, size),)].astype(jnp.int32).astype(jnp.float32) * scale


def sweep_kernel(
    sizes, owner_hbm, column_hbm, uf_hbm, counts_hbm, items_hbm, ratings_hbm, x_ref, r_ref,
    vbuf, rbuf, start, pcur, part, sent, recv, tot, leaving, last, p_ref, res_ref, xacc, damp_ref, counts_ref,
    ids, places, pos_ref, user_sem, count_sem, id_sem, place_sem, item_sem, rating_sem, i_send, i_recv,
    v_send, v_recv, d_send, d_recv, t_send, t_recv,
    g_send, g_recv, in_send, in_recv, out_send, f_send, f_recv,
):
    rows, cols, fibers = sizes
    half = cols // 2
    my_row, my_col, my_fiber = lax.axis_index("row"), lax.axis_index("col"), lax.axis_index("fiber")
    held_items = items_hbm.shape[0]
    share = held_items // fibers
    parts = 2 if rows == 4 and share % 2 == 0 else 1
    piece = share // parts
    held_blocks, block = ratings_hbm.shape[0], ratings_hbm.shape[1]
    own_users = uf_hbm.shape[0] // block
    slots = cols * own_users
    per_user = pos_ref.shape[1] // slots
    chunk = held_blocks // CHUNKS

    left = 1 - lax.div(my_col, half)
    depth = left * my_col + (1 - left) * (cols - 1 - my_col)
    inner = my_col + 2 * left - 1
    outer = my_col - 2 * left + 1
    side = lax.div(depth + 1, half)

    def row_of(d):
        return lax.rem(my_row + d, rows)

    def col_of(d):
        return lax.rem(my_col + d, cols)

    def fiber_of(d):
        return lax.rem(my_fiber + d, fibers)

    id_loads = [
        pltpu.make_async_copy(source, ids.at[my_fiber, i], id_sem.at[i])
        for i, source in enumerate((owner_hbm, column_hbm))
    ]
    for load in id_loads:
        load.start()
    item_load = pltpu.make_async_copy(items_hbm, vbuf.at[pl.ds(my_row * held_items, held_items)], item_sem)
    item_load.start()
    user_load = pltpu.make_async_copy(uf_hbm, x_ref, user_sem)
    user_load.start()
    count_load = pltpu.make_async_copy(counts_hbm, counts_ref, count_sem)
    count_load.start()

    def held_chunk(i):
        return pl.ds(my_fiber * held_blocks + i * chunk, chunk)

    rating_loads = []
    for i in range(CHUNKS):
        load = pltpu.make_async_copy(
            ratings_hbm.at[pl.ds(i * chunk, chunk)], rbuf.at[held_chunk(i)], rating_sem.at[i]
        )
        load.start()
        rating_loads.append(load)

    barrier = pltpu.get_barrier_semaphore()
    for d in range(1, rows):
        pl.semaphore_signal(barrier, inc=1, device_id={"row": row_of(d)}, device_id_type=MESH)
    for d in range(1, cols):
        pl.semaphore_signal(barrier, inc=1, device_id={"col": col_of(d)}, device_id_type=MESH)
    for d in range(1, fibers):
        pl.semaphore_signal(barrier, inc=1, device_id={"fiber": fiber_of(d)}, device_id_type=MESH)

    user_load.wait()
    for j in range(own_users):
        start[my_col * own_users + j] = x_ref[pl.ds(j * block, block), :].astype(jnp.bfloat16)
    for load in id_loads:
        load.wait()
    item_load.wait()
    pl.semaphore_wait(barrier, rows + cols + fibers - 3)

    id_sends = []
    for e in range(1, fibers):
        copy = pltpu.make_async_remote_copy(
            src_ref=ids.at[my_fiber],
            dst_ref=ids.at[my_fiber],
            send_sem=i_send.at[e],
            recv_sem=i_recv.at[e],
            device_id={"fiber": fiber_of(e)},
            device_id_type=MESH,
        )
        copy.start()
        id_sends.append(copy)

    def item_piece(row, i):
        return pl.ds(row * held_items + my_fiber * share + i * piece, piece)

    def item_copy(source, d, i, target):
        return pltpu.make_async_remote_copy(
            src_ref=vbuf.at[item_piece(source, i)],
            dst_ref=vbuf.at[item_piece(source, i)],
            send_sem=v_send.at[d, i],
            recv_sem=v_recv.at[d, i],
            device_id={"row": target},
            device_id_type=MESH,
        )

    if parts == 2:
        across = my_row + 1 - 2 * lax.rem(my_row, 2)
        along = my_row + 2 - 4 * lax.div(my_row, 2)
        corner = 3 - my_row
        peers = [my_row, across, along, corner]
        first = [item_copy(my_row, 1, 0, across), item_copy(my_row, 2, 1, along)]
        first += [item_copy(my_row, 1, 1, across), item_copy(my_row, 2, 0, along)]
        relays = [
            (item_copy(across, 1, 0, across), item_copy(across, 3, 0, along)),
            (item_copy(along, 2, 1, along), item_copy(along, 3, 1, across)),
        ]
        landed = [(1, 1), (2, 0), (3, 0), (3, 1)]
    else:
        peers = [lax.rem(my_row + rows - d, rows) for d in range(rows)]
        first = [item_copy(my_row, d, 0, row_of(d)) for d in range(1, rows)]
        relays = []
        landed = [(d, 0) for d in range(1, rows)]
    for copy in first:
        copy.start()
    item_sends = first + [onward for _, onward in relays]

    def start_copy(source, d, j):
        slot = source * own_users + j
        return pltpu.make_async_remote_copy(
            src_ref=start.at[slot],
            dst_ref=start.at[slot],
            send_sem=g_send.at[d, j],
            recv_sem=g_recv.at[slot],
            device_id={"col": col_of(d)},
            device_id_type=MESH,
        )

    for d in range(1, cols):
        for j in range(own_users):
            start_copy(my_col, d, j).start()
    rating_sends = []
    for i in range(CHUNKS):
        rating_loads[i].wait()
        for e in range(1, fibers):
            copy = pltpu.make_async_remote_copy(
                src_ref=rbuf.at[held_chunk(i)],
                dst_ref=rbuf.at[held_chunk(i)],
                send_sem=t_send.at[e, i],
                recv_sem=t_recv.at[e, i],
                device_id={"fiber": fiber_of(e)},
                device_id_type=MESH,
            )
            copy.start()
            rating_sends.append(copy)

    count_load.wait()
    damp_ref[...] = jnp.zeros_like(damp_ref)
    xacc[...] = jnp.zeros_like(xacc)
    for j in range(own_users):
        scaled = reg_weight * counts_ref[pl.ds(j, 1), :].astype(jnp.float32)
        across = jnp.broadcast_to(scaled, (block, block))
        own = my_col * own_users + j
        damp_ref[own] = jnp.broadcast_to(jnp.transpose(across)[:, :1], (block, damp_ref.shape[2]))
        xacc[own] = x_ref[pl.ds(j * block, block), :]

    for copy in id_sends:
        copy.wait_recv()
    total_blocks = fibers * held_blocks
    lanes = (held_blocks, held_blocks)
    here = lax.broadcasted_iota(jnp.int32, lanes, 0)
    lane = lax.broadcasted_iota(jnp.int32, lanes, 1)
    group = own_users * per_user
    ahead = sum(jnp.where(lane >= c * group, 1, 0) for c in range(1, cols))
    wanted = lane + (ahead * (fibers - 1) + my_fiber) * group
    keys = [jnp.broadcast_to(ids[e, 0], lanes) * total_blocks + lane + e * held_blocks for e in range(fibers)]
    standing = [jnp.transpose(key) for key in keys]
    found_place = jnp.zeros((1, held_blocks), jnp.int32)
    found_item = jnp.zeros((1, held_blocks), jnp.int32)
    for e in range(fibers):
        before = sum(jnp.where(other < keys[e], 1, 0) for other in standing)
        rank = jnp.sum(before, axis=0, keepdims=True)
        match = jnp.transpose(jnp.broadcast_to(rank, lanes)) == wanted
        column = jnp.transpose(jnp.broadcast_to(ids[e, 1], lanes))
        found_place += jnp.sum(jnp.where(match, here + e * held_blocks, 0), axis=0, keepdims=True)
        found_item += jnp.sum(jnp.where(match, column, 0), axis=0, keepdims=True)
    places[0:1, :] = found_place
    places[1:2, :] = found_item
    place_copy = pltpu.make_async_copy(places, pos_ref, place_sem)
    place_copy.start()

    shared = []

    def share_piece(d, i):
        for e in range(1, fibers):
            copy = pltpu.make_async_remote_copy(
                src_ref=vbuf.at[item_piece(peers[d], i)],
                dst_ref=vbuf.at[item_piece(peers[d], i)],
                send_sem=d_send.at[d, i, e],
                recv_sem=d_recv.at[d, i, e],
                device_id={"fiber": fiber_of(e)},
                device_id_type=MESH,
            )
            copy.start()
            shared.append(copy)

    for arrived, onward in relays:
        arrived.wait_recv()
        onward.start()
    if parts == 2:
        share_piece(1, 0)
        share_piece(2, 1)
    for d, i in landed:
        item_copy(peers[d], d, i, my_row).wait_recv()
        share_piece(d, i)
    place_copy.wait()
    for copy in rating_sends + shared:
        copy.wait_recv()

    cut_rows = block // CUTS

    def inward(stage, u, h):
        return pltpu.make_async_remote_copy(
            src_ref=sent.at[stage, u, h],
            dst_ref=recv.at[side, stage, u, h],
            send_sem=in_send.at[stage, u, h],
            recv_sem=in_recv.at[side, stage, u, h],
            device_id={"col": inner},
            device_id_type=MESH,
        )

    def outward(stage, u, h):
        return pltpu.make_async_remote_copy(
            src_ref=tot.at[stage, u, h],
            dst_ref=recv.at[1, stage, u, h],
            send_sem=out_send.at[stage, u, h],
            recv_sem=in_recv.at[1, stage, u, h],
            device_id={"col": outer},
            device_id_type=MESH,
        )

    def arrival(which, stage, u, h):
        return pltpu.make_async_remote_copy(
            src_ref=sent.at[stage, u, h],
            dst_ref=recv.at[which, stage, u, h],
            send_sem=in_send.at[stage, u, h],
            recv_sem=in_recv.at[which, stage, u, h],
            device_id={"col": inner},
            device_id_type=MESH,
        )

    def terms(stage, u):
        rows_of_user = start[u] if stage == 0 else pcur[u]
        base = u * per_user
        items = jnp.concatenate([vbuf[pos_ref[1, base + i]] for i in range(per_user)], axis=0)
        ratings = jnp.concatenate([rbuf[pos_ref[0, base + i]] for i in range(per_user)], axis=1)
        predicted = lax.dot_general(
            rows_of_user, items, (((1,), (1,)), ((), ())), preferred_element_type=jnp.float32
        )
        ratings = ratings.astype(jnp.float32)
        if stage == 0:
            weights = jnp.where(ratings != 0, ratings - predicted, 0.0)
        else:
            weights = jnp.where(ratings != 0, predicted, 0.0)
        total = jnp.dot(weights.astype(jnp.bfloat16), items, preferred_element_type=jnp.float32)
        if stage == 0:
            return total - damp_ref[u] * xacc[u]
        return total + damp_ref[u] * p_ref[u]

    def deliver(d, j, target, source):
        return pltpu.make_async_remote_copy(
            src_ref=leaving.at[target * own_users + j],
            dst_ref=last.at[source, j],
            send_sem=f_send.at[d, j],
            recv_sem=f_recv.at[source, j],
            device_id={"col": target},
            device_id_type=MESH,
        )

    def compute(stage, u):
        part[u] = terms(stage, u)
        if stage == ITERS:
            @pl.when(my_col != u // own_users)
            def _():
                store_coded(leaving, (u,), part[u])
                deliver(u // own_users, u % own_users, u // own_users, my_col).start()

            return

        @pl.when(depth == 0)
        def _():
            for h in range(CUTS):
                store_coded(sent, (stage, u, h), part[u, pl.ds(h * cut_rows, cut_rows)])
                inward(stage, u, h).start()

    def pass_on(stage, u):
        @pl.when(depth > 0)
        def _():
            for h in range(CUTS):
                arrival(0, stage, u, h).wait_recv()
                mine = part[u, pl.ds(h * cut_rows, cut_rows)]
                store_coded(sent, (stage, u, h), mine + load_coded(recv, (0, stage, u, h)))
                inward(stage, u, h).start()

    def collect(stage, u):
        @pl.when(depth == half - 1)
        def _():
            for h in range(CUTS):
                arrival(1, stage, u, h).wait_recv()
                both = load_coded(sent, (stage, u, h)) + load_coded(recv, (1, stage, u, h))
                store_coded(tot, (stage, u, h), both)
                if half > 1:
                    outward(stage, u, h).start()

        @pl.when(depth < half - 1)
        def _():
            for h in range(CUTS):
                arrival(1, stage, u, h).wait_recv()
                tot[stage, u, h] = recv[1, stage, u, h]

                @pl.when(depth > 0)
                def _():
                    outward(stage, u, h).start()

    def update(stage, u, image=None):
        if stage < ITERS:
            image = jnp.concatenate([load_coded(tot, (stage, u, h)) for h in range(CUTS)], axis=0)
        if stage == 0:
            res_ref[u] = image
            p_ref[u] = image
            pcur[u] = image.astype(jnp.bfloat16)
            return
        direction = p_ref[u]
        residual = res_ref[u]
        square = jnp.sum(residual * residual, axis=1, keepdims=True)
        step_size = square / (jnp.sum(direction * image, axis=1, keepdims=True) + tiny)
        residual = residual - step_size * image
        res_ref[u] = residual
        xacc[u] = xacc[u] + step_size * direction
        if stage < ITERS:
            renewed = jnp.sum(residual * residual, axis=1, keepdims=True)
            direction = residual + renewed / (square + tiny) * direction
            p_ref[u] = direction
            pcur[u] = direction.astype(jnp.bfloat16)

    order = sorted(range(cols), key=lambda c: (-abs(2 * c - cols + 1), c))
    order = [c * own_users + j for j in range(own_users) for c in order]
    for u in order:
        @pl.when(my_col != u // own_users)
        def _():
            start_copy(u // own_users, 1, u % own_users).wait_recv()

        compute(0, u)
    for stage in range(ITERS):
        for step in range(slots + LAG):
            if step < slots:
                pass_on(stage, order[step])
            if step >= LAG:
                u = order[step - LAG]
                collect(stage, u)
                update(stage, u)
                compute(stage + 1, u)
    for j in range(own_users):
        own = my_col * own_users + j
        image = part[own]
        for d in range(1, cols):
            source = col_of(d)
            deliver(d, j, my_col, source).wait_recv()
            image = image + load_coded(last, (source, j))
        update(ITERS, own, image)
        users = pl.ds(j * block, block)
        x_ref[users, :] = xacc[own]
        r_ref[users, :] = res_ref[own]

    for copy in item_sends + rating_sends + shared + id_sends:
        copy.wait_send()
    for d in range(1, cols):
        for j in range(own_users):
            start_copy(my_col, d, j).wait_send()
            deliver(col_of(d), j, col_of(d), my_col).wait_send()
    for stage in range(ITERS):
        for u in order:
            for h in range(CUTS):
                inward(stage, u, h).wait_send()

    @pl.when(depth > 0)
    def _():
        for stage in range(ITERS):
            for u in order:
                for h in range(CUTS):
                    outward(stage, u, h).wait_send()


def per_device(sizes, user_factors, item_factors, ratings, block_user, block_item, counts):
    rows, cols, fibers = sizes
    held_blocks, block = ratings.shape[2], ratings.shape[3]
    rank = user_factors.shape[1]
    users = user_factors.shape[0]
    own_users = users // block
    item_blocks = item_factors.shape[0] // block

    slots = cols * own_users
    dma = pltpu.SemaphoreType.DMA
    vmem = pl.BlockSpec(memory_space=pltpu.VMEM)
    hbm = pl.BlockSpec(memory_space=pl.ANY)
    return hand_out(*pl.pallas_call(
        functools.partial(sweep_kernel, sizes),
        out_shape=(
            jax.ShapeDtypeStruct((users, rank), jnp.float32),
            jax.ShapeDtypeStruct((users, rank), jnp.float32),
        ),
        in_specs=[hbm] * 6,
        out_specs=(vmem, vmem),
        scratch_shapes=[
            pltpu.VMEM((rows * item_blocks, block, rank), jnp.bfloat16),
            pltpu.VMEM((fibers * held_blocks, block, block), jnp.bfloat16),
            pltpu.VMEM((slots, block, rank), jnp.bfloat16),
            pltpu.VMEM((slots, block, rank), jnp.bfloat16),
            pltpu.VMEM((slots, block, rank), jnp.float32),
            pltpu.VMEM((ITERS, slots, CUTS, block // CUTS + pad, rank), jnp.int16),
            pltpu.VMEM((2, ITERS, slots, CUTS, block // CUTS + pad, rank), jnp.int16),
            pltpu.VMEM((ITERS, slots, CUTS, block // CUTS + pad, rank), jnp.int16),
            pltpu.VMEM((slots, block + pad, rank), jnp.int16),
            pltpu.VMEM((cols, own_users, block + pad, rank), jnp.int16),
            pltpu.VMEM((slots, block, rank), jnp.float32),
            pltpu.VMEM((slots, block, rank), jnp.float32),
            pltpu.VMEM((slots, block, rank), jnp.float32),
            pltpu.VMEM((slots, block, rank), jnp.float32),
            pltpu.VMEM((own_users, block), jnp.int32),
            pltpu.VMEM((fibers, 2, 1, held_blocks), jnp.int32),
            pltpu.VMEM((2, held_blocks), jnp.int32),
            pltpu.SMEM((2, held_blocks), jnp.int32),
            dma,
            dma,
            dma((2,)),
            dma,
            dma,
            dma((CHUNKS,)),
            dma((fibers,)),
            dma((fibers,)),
            dma((rows, 2)),
            dma((rows, 2)),
            dma((rows, 2, fibers)),
            dma((rows, 2, fibers)),
            dma((fibers, CHUNKS)),
            dma((fibers, CHUNKS)),
            dma((cols, own_users)),
            dma((slots,)),
            dma((ITERS, slots, CUTS)),
            dma((2, ITERS, slots, CUTS)),
            dma((ITERS, slots, CUTS)),
            dma((cols, own_users)),
            dma((cols, own_users)),
        ],
        compiler_params=pltpu.CompilerParams(
            collective_id=0, has_side_effects=True, vmem_limit_bytes=67043328
        ),
    )(
        block_user[0],
        block_item[0],
        user_factors,
        counts.reshape(own_users, block),
        item_factors.reshape(item_blocks, block, rank),
        ratings[0, 0],
    ))


def tail_kernel(x_ref, r_ref, xo_ref, ro_ref, sems):
    a = pltpu.make_async_copy(x_ref, xo_ref, sems.at[0])
    b = pltpu.make_async_copy(r_ref, ro_ref, sems.at[1])
    a.start()
    b.start()
    a.wait()
    b.wait()


def hand_out(x, r):
    vmem = pl.BlockSpec(memory_space=pltpu.VMEM)
    hbm = pl.BlockSpec(memory_space=pl.ANY)
    return pl.pallas_call(
        tail_kernel,
        out_shape=(jax.ShapeDtypeStruct(x.shape, x.dtype), jax.ShapeDtypeStruct(r.shape, r.dtype)),
        in_specs=[vmem, vmem],
        out_specs=(hbm, hbm),
        scratch_shapes=[pltpu.SemaphoreType.DMA((2,))],
    )(x, r)


def solution(mesh):
    sizes = (mesh.shape["row"], mesh.shape["col"], mesh.shape["fiber"])

    def whole(user_factors, item_factors, ratings, block_user, block_item, counts):
        return jax.shard_map(
            functools.partial(per_device, sizes),
            mesh=mesh,
            in_specs=(
                P(("row", "col", "fiber"), None),
                P(("row", "col"), None),
                P("row", "col", "fiber", None, None),
                P("row", "col", "fiber"),
                P("row", "col", "fiber"),
                P(("row", "col", "fiber")),
            ),
            out_specs=(P(("row", "col", "fiber"), None), P(("row", "col", "fiber"), None)),
            check_vma=False,
        )(user_factors, item_factors, ratings, block_user, block_item, counts)

    return whole
```
